256 devices in a mesh: dp: 64 (over z_lo, x, y), tensor: 4 (over z_hi, core).
Axes of the slice: x: 4, y: 4, z: 8 (z_hi: 2, z_lo: 4; z = z_hi * 4 + z_lo), core: 2. Of those that a mesh axis runs over, the one named last changes fastest.
Arguments:
- hidden_states: float32 [32768, 2048], P(('dp', 'tensor')), may hold values from -40 to 40
- lengths: int32 [64], P('dp'), may hold values from 128 to 512
- shard_order: int32 [64], replicated, may hold values from 0 to 63, each once
- gain_attn: float32 [2048], replicated, may hold values from 0.25 to 1.75
- w_query: bfloat16 [2048, 2048], P('dp', 'tensor'), may hold values from -0.015625 to 0.015625
- w_key: bfloat16 [2048, 2048], P('dp', 'tensor'), may hold values from -0.125 to 0.125
- w_value: bfloat16 [2048, 2048], P('dp', 'tensor'), may hold values from -0.125 to 0.125
- w_out: bfloat16 [2048, 2048], P('tensor', 'dp'), may hold values from -1 to 1
- rel_bias: float32 [32, 32], P(None, 'tensor'), may hold values from -6 to 300
- gain_ff: float32 [2048], replicated, may hold values from 0.25 to 1.75
- w_gate: bfloat16 [2048, 5120], P('dp', 'tensor'), may hold values from -0.125 to 0.125
- w_up: bfloat16 [2048, 5120], P('dp', 'tensor'), may hold values from -0.125 to 0.125
- w_down: bfloat16 [5120, 2048], P('tensor', 'dp'), may hold values from -0.078125 to 0.078125
- gain_final: float32 [2048], replicated, may hold values from 0.25 to 1.75
- w_reward: float32 [2048], replicated, may hold values from -0.125 to 0.125
Outputs:
- layer_output: float32 [32768, 2048], P(('dp', 'tensor'))
- normalized_rewards: float32 [64], P('dp')
The draws below stay inside these ranges and needn't reach their ends.
Inputs may be any that keep to these rules, and one draw needn't show every extreme that they name: `shard_order`: each of 0 to 64 - 1 appears once. `lengths`: positions at or beyond a rollout's length are padding.
All inputs are finite; a program needn't handle non-finite values.
Results may differ from the reference program's by a relative error of at most 0.02.
Values may be sent and summed in bfloat16 or wider, within the bound.
A program may use at most 128 MiB of HBM per device.

```python
import math
import jax
import jax.numpy as jnp
from jax import lax

D = 2048
HEADS = 32
DK = 64
FF = 5120
BUCKETS = 32
LEN = 512
SEQS = 64
TOKENS = 32768
N_DP = 64
N_TENSOR = 4


def draw_hidden_states(key, part):
    subkeys = jax.random.split(key, 3)
    base_draw = jnp.clip(jax.random.normal(subkeys[0], (TOKENS, D), jnp.float32), -4.0, 4.0)
    row_scale = jnp.exp(jax.random.uniform(subkeys[1], (TOKENS, 1), jnp.float32, math.log(0.3), math.log(3.0)))
    column_scale = jnp.exp(jax.random.uniform(subkeys[2], (1, D), jnp.float32, math.log(0.3), math.log(3.0)))
    return base_draw * row_scale * column_scale


def draw_rel_bias(key, part):
    subkeys = jax.random.split(key, 1)
    base_draw = jnp.clip(jax.random.normal(subkeys[0], (BUCKETS, HEADS), jnp.float32), -6.0, 6.0)
    return base_draw


def touch_ends(drawn, own_key, smallest, high):
    shape = drawn.shape
    place = [jax.random.randint(jax.random.fold_in(own_key, axis), (), 0, shape[axis]) for axis in range(len(shape))]
    drawn = drawn.at[tuple(place)].set(smallest)
    longest = shape.index(max(shape))
    place[longest] = (place[longest] + 1) % shape[longest]
    return drawn.at[tuple(place)].set(high)


def shard_levels(own_key, shape, cuts, low, largest):
    def one(position, blocks):
        steps = jax.random.uniform(jax.random.fold_in(jax.random.fold_in(own_key, 6), position), (blocks,), jnp.float32, low / len(cuts), largest / len(cuts))
        return jnp.repeat(jnp.exp(steps), shape[position] // blocks).reshape((-1,) + (1,) * (len(shape) - position - 1))

    gain = one(*cuts[0])
    for cut in cuts[1:]:
        gain = gain * one(*cut)
    return gain


def centred(rng, dims, scale, bound, pieces=(), held_as=jnp.bfloat16):
    loudness = shard_levels(rng, dims, pieces, -0.22, 0.18) if pieces else 1.0
    drawn = jax.random.normal(rng, dims, jnp.float32) * scale * loudness
    return jnp.minimum(jnp.maximum(drawn, -bound), bound).astype(held_as)


def setup_inputs(seed: int = 0) -> dict:
    arg_keys = jax.random.split(jax.random.key(seed), 16)
    return {
        "hidden_states": draw_hidden_states(jax.random.fold_in(arg_keys[15], 71), 0),
        "lengths": touch_ends(jax.random.randint(arg_keys[1], (SEQS,), LEN // 4, LEN + 1), jax.random.fold_in(arg_keys[1], 1), LEN // 4, LEN).astype(jnp.int32),
        "shard_order": jax.random.permutation(arg_keys[2], N_DP).astype(jnp.int32),
        "gain_attn": jnp.clip(1.0 + 0.15 * jax.random.normal(arg_keys[3], (D,), jnp.float32), 0.25, 1.75),
        "w_query": centred(arg_keys[4], (D, HEADS * DK), (D * DK) ** -0.5, 0.015625, ((0, 64), (1, 4))),
        "w_key": centred(arg_keys[5], (D, HEADS * DK), D ** -0.5, 0.125, ((0, 64), (1, 4))),
        "w_value": centred(arg_keys[6], (D, HEADS * DK), D ** -0.5, 0.125, ((0, 64), (1, 4))),
        "w_out": centred(arg_keys[7], (HEADS * DK, D), (HEADS * DK // 64) ** -0.5, 1.0, ((0, 4), (1, 64))),
        "rel_bias": draw_rel_bias(jax.random.fold_in(arg_keys[15], 71), 0),
        "gain_ff": jnp.clip(1.0 + 0.15 * jax.random.normal(arg_keys[9], (D,), jnp.float32), 0.25, 1.75),
        "w_gate": centred(arg_keys[10], (D, FF), D ** -0.5, 0.125, ((0, 64), (1, 4))),
        "w_up": centred(arg_keys[11], (D, FF), D ** -0.5, 0.125, ((0, 64), (1, 4))),
        "w_down": centred(arg_keys[12], (FF, D), FF ** -0.5, 0.078125, ((0, 4), (1, 64))),
        "gain_final": jnp.clip(1.0 + 0.15 * jax.random.normal(arg_keys[13], (D,), jnp.float32), 0.25, 1.75),
        "w_reward": centred(arg_keys[14], (D,), D ** -0.5, 0.125, (), jnp.float32),
    }


bucket_edges = (12, 16, 23, 32, 46, 64, 91)

def bucket_index(relative):
    distance = jnp.abs(relative)
    bucket_low = jnp.minimum(distance, 8)
    for threshold in bucket_edges:
        bucket_low = bucket_low + (distance >= threshold).astype(jnp.int32)
    return (jnp.where(relative > 0, 16, 0) + bucket_low).astype(jnp.int32)

def rms_norm(values_in, weight_gain):
    return values_in * lax.rsqrt(lax.optimization_barrier(jnp.mean(values_in * values_in, axis=-1, keepdims=True)) + 1e-06) * weight_gain

def restore_rows(matrix, inverse):
    blocks = matrix.reshape(N_DP, matrix.shape[0] // N_DP, matrix.shape[1])
    return jnp.take(blocks, inverse, axis=0).reshape(matrix.shape)

def restore_columns(matrix, inverse):
    blocks = matrix.reshape(matrix.shape[0], N_DP, matrix.shape[1] // N_DP)
    return jnp.take(blocks, inverse, axis=1).reshape(matrix.shape)

def group_sum(left, right):
    inner = left.shape[1] // N_TENSOR
    left_groups = left.reshape(left.shape[0], N_TENSOR, inner).astype(jnp.float32)
    right_groups = right.reshape(N_TENSOR, inner, right.shape[1]).astype(jnp.float32)
    partials = jnp.einsum('ljc,jcd->jld', left_groups, right_groups).astype(jnp.bfloat16)
    partials = lax.optimization_barrier(partials)
    return lax.optimization_barrier(jnp.sum(partials.astype(jnp.float32), axis=0))

def reference(hidden_states, lengths, shard_order, gain_attn, w_query, w_key, w_value, w_out, rel_bias, gain_ff, w_gate, w_up, w_down, gain_final, w_reward):
    inverse = jnp.argsort(shard_order).astype(jnp.int32)
    query_true = restore_rows(w_query, inverse)
    key_true = restore_rows(w_key, inverse)
    value_true = restore_rows(w_value, inverse)
    gate_true = restore_rows(w_gate, inverse)
    up_true = restore_rows(w_up, inverse)
    out_true = restore_columns(w_out, inverse)
    down_true = restore_columns(w_down, inverse)
    positions = jnp.arange(LEN, dtype=jnp.int32)
    relative = positions[None, :] - positions[:, None]
    position_bias = jnp.transpose(rel_bias[bucket_index(relative)], (2, 0, 1))

    def sequence_step(operands):
        states, length = operands
        normed = rms_norm(states, gain_attn).astype(jnp.bfloat16)
        queries = jnp.dot(normed, query_true, preferred_element_type=jnp.float32).astype(jnp.bfloat16)
        key_states = jnp.dot(normed, key_true, preferred_element_type=jnp.float32).astype(jnp.bfloat16)
        value_states = jnp.dot(normed, value_true, preferred_element_type=jnp.float32).astype(jnp.bfloat16)
        query_heads = queries.reshape(LEN, HEADS, DK).astype(jnp.float32)
        key_heads = key_states.reshape(LEN, HEADS, DK).astype(jnp.float32)
        value_heads = value_states.reshape(LEN, HEADS, DK).astype(jnp.float32)
        scores = jnp.einsum('qhd,khd->hqk', query_heads, key_heads) + position_bias
        in_range = positions < length
        scores = jnp.where(in_range[None, None, :], scores, -1e+30)
        row_max = lax.optimization_barrier(jnp.max(scores, axis=-1, keepdims=True))
        exp_scores = jnp.exp(scores - row_max)
        soft_weights = (exp_scores / lax.optimization_barrier(jnp.sum(exp_scores, axis=-1, keepdims=True))).astype(jnp.bfloat16)
        context = jnp.einsum('hqk,khd->qhd', soft_weights.astype(jnp.float32), value_heads)
        context = context.astype(jnp.bfloat16).reshape(LEN, HEADS * DK)
        mid = states + group_sum(context, out_true)
        mid_normed = rms_norm(mid, gain_ff).astype(jnp.bfloat16)
        gate_proj = jnp.dot(mid_normed, gate_true, preferred_element_type=jnp.float32)
        up_proj = jnp.dot(mid_normed, up_true, preferred_element_type=jnp.float32)
        activated = (jax.nn.gelu(gate_proj, approximate=True) * up_proj).astype(jnp.bfloat16)
        layer_output = mid + group_sum(activated, down_true)
        final_normed = rms_norm(layer_output, gain_final)
        token_score = jnp.dot(final_normed, w_reward, precision=lax.Precision.HIGHEST)
        pooled_sum = jnp.sum(jnp.where(in_range, token_score, 0.0))
        return (layer_output, pooled_sum / length.astype(jnp.float32))
    sequences = hidden_states.reshape(SEQS, LEN, D)
    outputs, rewards = lax.map(sequence_step, (sequences, lengths))
    reward_mean = jnp.mean(rewards)
    reward_var = jnp.mean((rewards - reward_mean) * (rewards - reward_mean))
    normalized = (rewards - reward_mean) / jnp.sqrt(reward_var + 1e-06)
    return (outputs.reshape(TOKENS, D), normalized)
```

```python
import jax
import jax.numpy as jnp
from jax import lax
from jax.sharding import PartitionSpec as P
from jax.experimental import pallas as pl
from jax.experimental.pallas import tpu as pltpu

DK = 64
LEN = 512


MESH = pl.DeviceIdType.MESH
CH = (768, 256, 640, 640, 640)
NC = len(CH)

def coords():
    d = lax.axis_index("dp"); t = lax.axis_index("tensor")
    return d // 16, (d // 4) % 4, d % 4, t // 2, t % 2

def did(z, x, y, h, c):
    return {"dp": z * 16 + x * 4 + y, "tensor": h * 2 + c}

def gather_kernel(*refs):
    src = refs[: 2 * NC]; gb = refs[2 * NC: 4 * NC]
    send_sem, recv_sem, loc_sem = refs[4 * NC:]
    z, x, y, h, c = coords()
    barrier = pltpu.get_barrier_semaphore()
    peers = [did((z + k) % 4, x, y, h, c) for k in (1, 2, 3)]
    peers += [did(z, (x + k) % 4, y, h, c) for k in (1, 3)]
    peers += [did(z, x, (y + k) % 4, h, c) for k in (1, 3)]
    for p in peers:
        pl.semaphore_signal(barrier, inc=1, device_id=p, device_id_type=MESH)
    pl.semaphore_wait(barrier, len(peers))
    base = (y * 16 + x * 4, x * 16 + y * 4)
    my1 = (x, y); my2 = (y, x)

    def nb(col, ph, k):
        if (col == 0) == (ph == 1):
            return did(z, (x + k) % 4, y, h, c)
        return did(z, x, (y + k) % 4, h, c)

    def sec(col, ph, k):
        if ph == 1:
            return my2[col] * 16 + ((my1[col] + k) % 4) * 4
        return ((my2[col] + k) % 4) * 16

    def send(col, ch, start, size, slot, dev):
        g = gb[col * NC + ch]
        pltpu.make_async_remote_copy(src_ref=g.at[pl.ds(start, size)], dst_ref=g.at[pl.ds(start, size)],
            send_sem=send_sem.at[col, ch], recv_sem=recv_sem.at[col, ch, slot],
            device_id=dev, device_id_type=MESH).start()

    def wait_recv(col, ch, slot, size):
        g = gb[col * NC + ch]
        pltpu.make_async_copy(g.at[pl.ds(0, size)], g.at[pl.ds(0, size)], recv_sem.at[col, ch, slot]).wait()

    def level(col, ch, lv):
        g = gb[col * NC + ch]; s = src[col * NC + ch]
        if lv == 0:
            mine = base[col] + z
            pltpu.make_async_copy(s, g.at[mine], loc_sem.at[col, ch]).start()
            for k in (1, 2, 3):
                pltpu.make_async_remote_copy(src_ref=s, dst_ref=g.at[mine], send_sem=send_sem.at[col, ch],
                    recv_sem=recv_sem.at[col, ch, 0], device_id=did((z + k) % 4, x, y, h, c), device_id_type=MESH).start()
        elif lv in (1, 3):
            ph = 1 if lv == 1 else 2
            if ph == 1:
                pltpu.make_async_copy(s, g.at[0], loc_sem.at[col, ch]).wait()
                wait_recv(col, ch, 0, 3)
            else:
                wait_recv(col, ch, 3, 4)
            size = 4 if ph == 1 else 16
            b = 1 if ph == 1 else 4
            for j, k in ((0, 1), (1, 3)):
                send(col, ch, sec(col, ph, 0), size, b + j, nb(col, ph, k))
        elif lv in (2, 4):
            ph = 1 if lv == 2 else 2
            size = 4 if ph == 1 else 16
            b = 1 if ph == 1 else 4
            half = size // 2
            wait_recv(col, ch, b, size)
            send(col, ch, sec(col, ph, 3), half, b + 2, nb(col, ph, 1))
            wait_recv(col, ch, b + 1, size)
            send(col, ch, sec(col, ph, 1) + half, half, b + 2, nb(col, ph, 3))
        else:
            wait_recv(col, ch, 6, 16)

    for t in range(NC + 5):
        for ch in range(NC):
            if 0 <= t - ch <= 5:
                for col in (0, 1):
                    level(col, ch, t - ch)
    for ch in range(NC):
        for col in (0, 1):
            g = gb[col * NC + ch]
            pltpu.make_async_copy(g.at[pl.ds(0, 63)], g.at[pl.ds(0, 63)], send_sem.at[col, ch]).wait()


ANY = pl.BlockSpec(memory_space=pl.ANY)
VM = pl.BlockSpec(memory_space=pltpu.VMEM)
def gather(*srcs):
    outs = [jax.ShapeDtypeStruct((64, 32, n), jnp.bfloat16) for _ in range(2) for n in CH]
    return pl.pallas_call(gather_kernel, out_shape=outs, in_specs=[ANY] * (2 * NC), out_specs=[VM] * (2 * NC),
        scratch_shapes=[pltpu.SemaphoreType.DMA((2, NC)), pltpu.SemaphoreType.DMA((2, NC, 7)), pltpu.SemaphoreType.DMA((2, NC))],
        compiler_params=pltpu.CompilerParams(collective_id=0, has_side_effects=True, vmem_limit_bytes=60 << 20), name="gather")(*srcs)


bucket_edges = (12, 16, 23, 32, 46, 64, 91)


def in_order(parts, dim):
    parts = jnp.moveaxis(parts, 0, dim)
    shape = parts.shape
    return parts.reshape(*shape[:dim], shape[dim] * shape[dim + 1], *shape[dim + 2 :])


def from_everyone(array, axis):
    peers = lax.axis_size(axis)
    return lax.all_to_all(
        jnp.broadcast_to(array[None], (peers, *array.shape)), axis, 0, 0, tiled=True
    )


def gather_directly(array, axis, dim):
    return in_order(from_everyone(array, axis), dim)


def in_one_piece(arrays, axis, dim, along):
    ends, at = ([], 0)
    for a in arrays[:-1]:
        at += a.shape[along]
        ends.append(at)
    both = jnp.concatenate(arrays, axis=along)
    return tuple(jnp.split(lax.all_gather(both, axis, axis=dim, tiled=True), ends, axis=along))


def cut_along(array, dim, peers):
    shape = array.shape
    parts = array.reshape(*shape[:dim], peers, shape[dim] // peers, *shape[dim + 1 :])
    return jnp.moveaxis(parts, dim, 0)


def sent_and_summed(array, axis, dim):
    peers = lax.axis_size(axis)
    parts = lax.all_to_all(cut_along(array, dim, peers), axis, 0, 0, tiled=True)
    return jnp.sum(parts.astype(jnp.float32), axis=0)


def of_everyone(array, axis):
    return from_everyone(array, axis).sum(axis=0)


def packed_total(arrays, axis):
    line, at, gathered = (jnp.concatenate([a.reshape(-1) for a in arrays]), 0, [])
    running = of_everyone(line, axis)
    for a in arrays:
        gathered.append(running[at : at + a.size].reshape(a.shape))
        at += a.size
    return tuple(gathered)


def bucket_index(relative):
    distance = jnp.abs(relative)
    bucket_low = jnp.minimum(distance, 8)
    for threshold in bucket_edges:
        bucket_low = bucket_low + (distance >= threshold).astype(jnp.int32)
    return jnp.where(relative > 0, 16, 0) + bucket_low


def rms_norm(values_in, weight_gain):
    return (
        values_in
        * lax.rsqrt(jnp.mean(values_in * values_in, axis=-1, keepdims=True) + 1e-06)
        * weight_gain
    )


def reorder_blocks(values_in, ordering):
    full_shape = values_in.shape
    blocks = values_in.reshape(
        full_shape[:-1] + (ordering.shape[0], full_shape[-1] // ordering.shape[0])
    )
    return jnp.take(blocks, ordering, axis=-2).reshape(full_shape)


def local(
    hidden_states,
    lengths,
    shard_order,
    gain_attn,
    w_query,
    w_key,
    w_value,
    w_out,
    rel_bias,
    gain_ff,
    w_gate,
    w_up,
    w_down,
    gain_final,
    w_reward,
):
    groups = shard_order.shape[0]
    block_ids = jnp.arange(groups, dtype=jnp.int32)
    inverse = jnp.sum(
        block_ids[:, None] * (shard_order[:, None] == block_ids[None, :]).astype(jnp.int32), axis=0
    )
    own_rows, attn_gain, feed_gain, final_gain, reward_head = (
        hidden_states, gain_attn, gain_ff, gain_final, w_reward)
    out_t, down_t = w_out.T, w_down.T
    halves = []
    for col in (0, 1):
        h = slice(col * 256, col * 256 + 256)
        half = slice(col * 640, col * 640 + 640)
        big = (w_gate, w_up)[col]
        halves += [jnp.concatenate([w_query[:, h], w_key[:, h], w_value[:, h]], axis=1), out_t[:, h],
                   big[:, :640], big[:, 640:], down_t[:, half]]
    got = gather(*halves)
    zs, xs, ys = inverse // 16, (inverse // 4) % 4, inverse % 4
    where = (ys * 16 + xs * 4 + zs, xs * 16 + ys * 4 + zs)

    def true(col, ch):
        blocks = jnp.take(got[col * NC + ch], where[col], axis=0)
        return blocks.reshape(64 * 32, blocks.shape[2])

    qkv = [true(0, 0), true(1, 0)]
    full = [jnp.concatenate([q[:, i * 256:(i + 1) * 256] for q in qkv], axis=1) for i in range(3)]
    out_full = jnp.concatenate([true(0, 1), true(1, 1)], axis=1)
    gate_full = jnp.concatenate([true(0, 2), true(0, 3)], axis=1)
    up_full = jnp.concatenate([true(1, 2), true(1, 3)], axis=1)
    down_full = jnp.concatenate([true(0, 4), true(1, 4)], axis=1)
    row_count = own_rows.shape[0]
    row_start = lax.axis_index("tensor") * row_count
    normed = gather_directly(rms_norm(own_rows, attn_gain).astype(jnp.bfloat16), "tensor", 0)

    def contract_with(source):

        def contract(running, portion, offset):
            return jnp.dot(source, portion, preferred_element_type=jnp.float32)

        return contract

    inner_width = w_query.shape[1]
    zero_block = jnp.zeros((LEN, inner_width), jnp.float32)
    attn_contract = contract_with(normed)
    running = (zero_block, zero_block, zero_block)
    portion = full
    offset = jnp.int32(0)
    queries = attn_contract(running[0], portion[0], offset)
    key_states = attn_contract(running[1], portion[1], offset)
    value_states = attn_contract(running[2], portion[2], offset)
    head_count = inner_width // DK
    query_heads = queries.astype(jnp.bfloat16).reshape(LEN, head_count, DK).transpose(1, 0, 2)
    key_heads = key_states.astype(jnp.bfloat16).reshape(LEN, head_count, DK).transpose(1, 0, 2)
    value_heads = value_states.astype(jnp.bfloat16).reshape(LEN, head_count, DK).transpose(1, 0, 2)
    span = 2 * LEN - 1
    offsets = jnp.arange(span, dtype=jnp.int32)
    relative = jnp.where(offsets < LEN, offsets, offsets - span)
    bucket_ids = bucket_index(relative)
    onehot = (
        bucket_ids[:, None] == jnp.arange(rel_bias.shape[0], dtype=jnp.int32)[None, :]
    ).astype(jnp.float32)
    offset_bias = jnp.dot(onehot, rel_bias, precision=lax.Precision.HIGHEST).T
    length = lengths[0]
    in_range = jnp.arange(LEN, dtype=jnp.int32) < length

    def head_step(operands):
        head_query, head_key, head_value, head_offsets = operands
        repeated = jnp.tile(head_offsets, LEN)[: LEN * (span - 1)].reshape(LEN, span - 1)[:, :LEN]
        scores = jnp.dot(head_query, head_key.T, preferred_element_type=jnp.float32) + repeated
        scores = jnp.where(in_range[None, :], scores, -1e30)
        row_max = jnp.max(scores, axis=-1, keepdims=True)
        exp_scores = jnp.exp(scores - row_max)
        soft_weights = (exp_scores / jnp.sum(exp_scores, axis=-1, keepdims=True)).astype(
            jnp.bfloat16
        )
        return jnp.dot(soft_weights, head_value, preferred_element_type=jnp.float32).astype(
            jnp.bfloat16
        )

    context = lax.map(head_step, (query_heads, key_heads, value_heads, offset_bias))
    context = context.transpose(1, 0, 2).reshape(LEN, inner_width)
    attn_partial = jnp.dot(
        context, out_full.T, preferred_element_type=jnp.float32
    ).astype(jnp.bfloat16)
    mid_own = own_rows + sent_and_summed(attn_partial, "tensor", 0)
    mid_normed = gather_directly(rms_norm(mid_own, feed_gain).astype(jnp.bfloat16), "tensor", 0)
    hidden_width = w_gate.shape[1]
    zero_hidden = jnp.zeros((LEN, hidden_width), jnp.float32)
    feed_contract = contract_with(mid_normed)
    running = (zero_hidden, zero_hidden)
    portion = (gate_full, up_full)
    offset = jnp.int32(0)
    gate_proj = feed_contract(running[0], portion[0], offset)
    up_proj = feed_contract(running[1], portion[1], offset)
    activated = (jax.nn.gelu(gate_proj, approximate=True) * up_proj).astype(jnp.bfloat16)
    feed_partial = jnp.dot(
        activated,
        down_full.T,
        preferred_element_type=jnp.float32,
    ).astype(jnp.bfloat16)
    output_rows = mid_own + lax.psum_scatter(
        feed_partial, "tensor", scatter_dimension=0, tiled=True
    ).astype(jnp.float32)
    final_normed = rms_norm(output_rows, final_gain)
    token_score = jnp.dot(final_normed, reward_head, precision=lax.Precision.HIGHEST)
    positions = row_start + jnp.arange(row_count, dtype=jnp.int32)
    local_pool = jnp.sum(jnp.where(positions < length, token_score, 0.0))
    pooled_sum = of_everyone(local_pool, "tensor")
    reward = jnp.reshape(pooled_sum / length.astype(jnp.float32), (1,))
    rollouts = lax.axis_size("dp") * lengths.shape[0]
    first_moment, second_moment = packed_total((jnp.sum(reward), jnp.sum(reward * reward)), "dp")
    reward_mean = first_moment / rollouts
    reward_var = second_moment / rollouts - reward_mean * reward_mean
    normalized = (reward - reward_mean) / jnp.sqrt(reward_var + 1e-06)
    return (output_rows, normalized)


def solution(mesh):
    placed = (
        P(("dp", "tensor"), None),
        P("dp"),
        P(),
        P(),
        P("dp", "tensor"),
        P("dp", "tensor"),
        P("dp", "tensor"),
        P("tensor", "dp"),
        P(None, "tensor"),
        P(),
        P("dp", "tensor"),
        P("dp", "tensor"),
        P("tensor", "dp"),
        P(),
        P(),
    )
    return jax.shard_map(
        local,
        mesh=mesh,
        in_specs=placed,
        out_specs=(P(("dp", "tensor"), None), P("dp")),
        check_vma=False,
    )
```

```python
import jax
import jax.numpy as jnp
from jax import lax
from jax.sharding import PartitionSpec as P
from jax.experimental import pallas as pl
from jax.experimental.pallas import tpu as pltpu

DK = 64
LEN = 512
D = 2048
ROWS = 128
MESH = pl.DeviceIdType.MESH
BF = jnp.bfloat16
F32 = jnp.float32
CH = (768, 256, 768, 512, 640)
NC = len(CH)
GA, GF = 2, 4
bucket_edges = (12, 16, 23, 32, 46, 64, 91)


def coords():
    d = lax.axis_index("dp")
    t = lax.axis_index("tensor")
    return d // 16, (d // 4) % 4, d % 4, t // 2, t % 2


def did(z, x, y, h, c):
    return {"dp": z * 16 + x * 4 + y, "tensor": h * 2 + c}


def rms(v, gain):
    return v * lax.rsqrt(jnp.mean(v * v, axis=-1, keepdims=True) + 1e-06) * gain


def nt(a, b):
    return lax.dot_general(a, b, (((1,), (1,)), ((), ())), preferred_element_type=F32)


def layer_kernel(*refs):
    (pos, length_ref, rel, hidden, gains), refs = refs[:5], refs[5:]
    src, refs = refs[: 2 * NC], refs[2 * NC :]
    (out, norm_out), refs = refs[:2], refs[2:]
    gb, refs = refs[: 2 * NC], refs[2 * NC :]
    (nbuf, mbuf, bias, qkv, ctx, act, part, mid, s1a, r1a, s2a, r2a, s1f, r1f, s2f, r2f, ra, rb) = refs[:18]
    send_sem, recv_sem, loc_sem, ag_send, ag_recv, ea_send, ea_recv, ef_send, ef_recv, rw_send, rw_recv = refs[18:]
    z, x, y, h, c = coords()
    me = h * 2 + c
    sib, far = did(z, x, y, h, 1 - c), did(z, x, y, 1 - h, c)
    i_sib, i_far, i_farsib = h * 2 + 1 - c, (1 - h) * 2 + c, (1 - h) * 2 + 1 - c
    length = length_ref[0]

    line = h * 8 + z * 2 + c
    plane = x * 4 + y

    def line_peer(k):
        i = (line + k) % 16
        return did((i // 2) % 4, x, y, i // 8, i % 2)

    def plane_peer(k):
        i = (plane + k) % 16
        return did(z, i // 4, i % 4, h, c)

    barrier = pltpu.get_barrier_semaphore()
    for k in range(1, 16):
        pl.semaphore_signal(barrier, inc=1, device_id=line_peer(k), device_id_type=MESH)
        pl.semaphore_signal(barrier, inc=1, device_id=plane_peer(k), device_id_type=MESH)
    pl.semaphore_wait(barrier, 30)

    base = (y * 16 + x * 4, x * 16 + y * 4)
    ring1, ring2 = (x, y), (y, x)

    def remote(s, d, ss, rs, dev):
        return pltpu.make_async_remote_copy(
            src_ref=s, dst_ref=d, send_sem=ss, recv_sem=rs, device_id=dev, device_id_type=MESH
        )

    def ring_peer(col, ph, k):
        if (col == 0) == (ph == 1):
            return did(z, (x + k) % 4, y, h, c)
        return did(z, x, (y + k) % 4, h, c)

    def section(col, ph, k):
        if ph == 1:
            return ring2[col] * 16 + ((ring1[col] + k) % 4) * 4
        return ((ring2[col] + k) % 4) * 16

    def send(col, ch, start, size, slot, dev):
        g = gb[col * NC + ch]
        s = g.at[pl.ds(start, size)]
        remote(s, s, send_sem.at[col, ch], recv_sem.at[col, ch, slot], dev).start()

    def arrived(ref, sem):
        pltpu.make_async_copy(ref, ref, sem).wait()

    def came(col, ch, slot, size):
        arrived(gb[col * NC + ch].at[pl.ds(0, size)], recv_sem.at[col, ch, slot])

    def level(col, ch, lv):
        g, s = gb[col * NC + ch], src[col * NC + ch]
        if lv == 0:
            mine = base[col] + z
            pltpu.make_async_copy(s, g.at[mine], loc_sem.at[col, ch]).start()
            for k in (1, 2, 3):
                remote(
                    s, g.at[mine], send_sem.at[col, ch], recv_sem.at[col, ch, 0], did((z + k) % 4, x, y, h, c)
                ).start()
        elif lv in (1, 3):
            ph = 1 if lv == 1 else 2
            if ph == 1:
                pltpu.make_async_copy(s, g.at[0], loc_sem.at[col, ch]).wait()
                came(col, ch, 0, 3)
            else:
                came(col, ch, 3, 4)
            size, b = (4, 1) if ph == 1 else (16, 4)
            for j, k in ((0, 1), (1, 3)):
                send(col, ch, section(col, ph, 0), size, b + j, ring_peer(col, ph, k))
        elif lv in (2, 4):
            ph = 1 if lv == 2 else 2
            size, b = (4, 1) if ph == 1 else (16, 4)
            half = size // 2
            came(col, ch, b, size)
            send(col, ch, section(col, ph, 3), half, b + 2, ring_peer(col, ph, 1))
            came(col, ch, b + 1, size)
            send(col, ch, section(col, ph, 1) + half, half, b + 2, ring_peer(col, ph, 3))
        else:
            came(col, ch, 6, 16)

    def wave(t):
        for ch in range(NC):
            if 0 <= t - ch <= 5:
                for col in (0, 1):
                    level(col, ch, t - ch)

    def spread(buf, n):
        to_sib = remote(buf.at[me], buf.at[me], ag_send.at[n, 0], ag_recv.at[n, 0], sib)
        to_far = remote(buf.at[me], buf.at[me], ag_send.at[n, 1], ag_recv.at[n, 1], far)
        to_far.start()
        to_sib.start()

    def pass_on(buf, n):
        arrived(buf.at[0], ag_recv.at[n, 1])
        remote(buf.at[i_far], buf.at[i_far], ag_send.at[n, 2], ag_recv.at[n, 2], sib).start()

    def spread_end(buf, n):
        arrived(buf.at[0], ag_recv.at[n, 0])
        arrived(buf.at[0], ag_recv.at[n, 2])

    def to_sibling(g, width, s1, r1, ss, rs):
        cols = slice(g * width, (g + 1) * width)
        s1[g, 0] = part[i_sib, :, cols].astype(BF)
        s1[g, 1] = part[i_farsib, :, cols].astype(BF)
        remote(s1.at[g], r1.at[g], ss.at[0, g], rs.at[0, g], sib).start()

    def to_far(g, width, r1, s2, r2, ss, rs):
        cols = slice(g * width, (g + 1) * width)
        arrived(r1.at[g], rs.at[0, g])
        s2[g] = (part[i_far, :, cols] + r1[g, 1].astype(F32)).astype(BF)
        remote(s2.at[g], r2.at[g], ss.at[1, g], rs.at[1, g], far).start()

    def total(g, width, r1, r2, rs):
        cols = slice(g * width, (g + 1) * width)
        arrived(r2.at[g], rs.at[1, g])
        return part[me, :, cols] + r1[g, 0].astype(F32) + r2[g].astype(F32)

    def blocks(col, ch, first, count, cols):
        g = gb[col * NC + ch]
        return jnp.concatenate([g[pos[col, first + b], :, cols] for b in range(count)], axis=0)

    wave(0)
    nbuf[me] = rms(hidden[...], gains[0:1]).astype(BF)
    spread(nbuf, 0)
    wave(1)

    row = lax.broadcasted_iota(jnp.int32, (ROWS, ROWS), 0)
    lane = lax.broadcasted_iota(jnp.int32, (ROWS, ROWS), 1)

    def bias_tile(n, _):
        for o in range(3):
            r = (o - 1) * ROWS + lane - row
            dist = jnp.abs(r)
            low = jnp.minimum(dist, 8)
            for edge in bucket_edges:
                low = low + (dist >= edge).astype(jnp.int32)
            bucket = jnp.where(r > 0, 16, 0) + low
            tile = jnp.zeros((ROWS, ROWS), F32)
            for b in range(32):
                tile = jnp.where(bucket == b, rel[b, n], tile)
            bias[n, o] = tile
        return 0

    lax.fori_loop(0, 8, bias_tile, 0)
    wave(2)
    wave(3)
    pass_on(nbuf, 0)
    wave(4)
    spread_end(nbuf, 0)
    wave(5)

    for col in (0, 1):
        def qkv_tile(i, _):
            cols = pl.ds(pl.multiple_of(i * 256, 256), 256)
            w = blocks(col, 0, 0, 64, cols)
            qkv[col, :, cols] = jnp.dot(
                nbuf[...].reshape(LEN, D), w, preferred_element_type=F32
            ).astype(BF)
            return 0

        lax.fori_loop(0, 3, qkv_tile, 0)

    lane_q = lax.broadcasted_iota(jnp.int32, (ROWS, 128), 1)
    key_pos = lax.broadcasted_iota(jnp.int32, (ROWS, LEN), 1)
    valid = key_pos < length

    def heads(p, _):
        col = p // 2
        at = (p % 2) * 128
        q_cols = pl.ds(pl.multiple_of(at, 128), 128)
        k_cols = pl.ds(pl.multiple_of(at + 256, 128), 128)
        v_cols = pl.ds(pl.multiple_of(at + 512, 128), 128)
        keys = qkv[col, :, k_cols]
        values = qkv[col, :, v_cols]
        for qt in range(4):
            q = qkv[col, qt * ROWS : (qt + 1) * ROWS, q_cols]
            got = []
            for hh in (0, 1):
                n = p * 2 + hh
                q_head = jnp.where((lane_q >= 64) == (hh == 1), q, jnp.zeros_like(q))
                s = nt(q_head, keys)
                tiles = []
                for kt in range(4):
                    if abs(kt - qt) <= 1:
                        tiles.append(bias[n, kt - qt + 1])
                    else:
                        tiles.append(jnp.full((ROWS, ROWS), rel[31 if kt > qt else 15, n], F32))
                s = jnp.where(valid, s + jnp.concatenate(tiles, axis=1), -1e30)
                e = jnp.exp(s - jnp.max(s, axis=-1, keepdims=True))
                pr = (e * (1.0 / jnp.sum(e, axis=-1, keepdims=True))).astype(BF)
                got.append(jnp.dot(pr, values, preferred_element_type=F32))
            c_cols = pl.ds(pl.multiple_of(p * 128, 128), 128)
            ctx[qt * ROWS : (qt + 1) * ROWS, c_cols] = jnp.where(lane_q < 64, got[0], got[1]).astype(BF)
        return 0

    lax.fori_loop(0, 2, heads, 0)
    wave(6)
    lax.fori_loop(2, 4, heads, 0)

    def out_tile(i, _):
        cols = pl.ds(pl.multiple_of(i * 256, 256), 256)
        all_ = slice(0, 256)
        s = nt(ctx[:, :256], blocks(0, 1, i * 8, 8, all_)) + nt(ctx[:, 256:], blocks(1, 1, i * 8, 8, all_))
        part[:, :, cols] = s.reshape(4, ROWS, 256)
        return 0

    wa = D // GA
    for g in range(GA):
        lax.fori_loop(g * (8 // GA), (g + 1) * (8 // GA), out_tile, 0)
        to_sibling(g, wa, s1a, r1a, ea_send, ea_recv)
    for g in range(GA):
        to_far(g, wa, r1a, s2a, r2a, ea_send, ea_recv)
    wave(7)
    for g in range(GA):
        cols = slice(g * wa, (g + 1) * wa)
        mid[:, cols] = hidden[:, cols] + total(g, wa, r1a, r2a, ea_recv)
    mbuf[me] = rms(mid[...], gains[1:2]).astype(BF)
    spread(mbuf, 1)
    wave(8)
    pass_on(mbuf, 1)
    spread_end(mbuf, 1)

    def feed_tile(ch, i, at):
        cols = pl.ds(pl.multiple_of(i * 256, 256), 256)
        lhs = mbuf[...].reshape(LEN, D)
        gate = jnp.dot(lhs, blocks(0, ch, 0, 64, cols), preferred_element_type=F32)
        up = jnp.dot(lhs, blocks(1, ch, 0, 64, cols), preferred_element_type=F32)
        act[:, pl.ds(pl.multiple_of(at + i * 256, 256), 256)] = (
            jax.nn.gelu(gate, approximate=True) * up
        ).astype(BF)
        return 0

    lax.fori_loop(0, 3, lambda i, _: feed_tile(2, i, 0), 0)
    lax.fori_loop(0, 2, lambda i, _: feed_tile(3, i, 768), 0)
    wave(9)

    def down_tile(i, _):
        cols = pl.ds(pl.multiple_of(i * 256, 256), 256)
        all_ = slice(0, 640)
        s = nt(act[:, :640], blocks(0, 4, i * 8, 8, all_)) + nt(act[:, 640:], blocks(1, 4, i * 8, 8, all_))
        part[:, :, cols] = s.reshape(4, ROWS, 256)
        return 0

    wf = D // GF
    for g in range(GF):
        lax.fori_loop(g * (8 // GF), (g + 1) * (8 // GF), down_tile, 0)
        to_sibling(g, wf, s1f, r1f, ef_send, ef_recv)
        if g > 0:
            to_far(g - 1, wf, r1f, s2f, r2f, ef_send, ef_recv)
    to_far(GF - 1, wf, r1f, s2f, r2f, ef_send, ef_recv)
    square = jnp.zeros((ROWS, 1), F32)
    dot = jnp.zeros((ROWS, 1), F32)
    for g in range(GF):
        cols = slice(g * wf, (g + 1) * wf)
        o = mid[:, cols] + total(g, wf, r1f, r2f, ef_recv)
        out[:, cols] = o
        square = square + jnp.sum(o * o, axis=-1, keepdims=True)
        dot = dot + jnp.sum(o * (gains[2:3, cols] * gains[3:4, cols]), axis=-1, keepdims=True)
    score = dot * lax.rsqrt(square * (1.0 / D) + 1e-06)
    at_row = lax.broadcasted_iota(jnp.int32, (ROWS, 1), 0) + me * ROWS
    pooled = jnp.sum(jnp.where(at_row < length, score, 0.0), axis=0, keepdims=True)

    ra[line] = jnp.broadcast_to(pooled / length.astype(F32), (8, 128))
    copies = []
    for k in range(1, 16):
        cp = remote(ra.at[line], ra.at[line], rw_send.at[0], rw_recv.at[0], line_peer(k))
        cp.start()
    arrived(ra.at[pl.ds(0, 15)], rw_recv.at[0])
    sub = lax.broadcasted_iota(jnp.int32, (8, 128), 0)
    tile = jnp.zeros((8, 128), F32)
    for k in range(4):
        tile = jnp.where(sub == k, ra[2 * k] + ra[2 * k + 1] + ra[8 + 2 * k] + ra[9 + 2 * k], tile)
    rb[plane] = tile
    for k in range(1, 16):
        remote(rb.at[plane], rb.at[plane], rw_send.at[1], rw_recv.at[1], plane_peer(k)).start()
    own = ra[2 * z] + ra[2 * z + 1] + ra[8 + 2 * z] + ra[9 + 2 * z]
    arrived(rb.at[pl.ds(0, 15)], rw_recv.at[1])
    every = jnp.sum(rb[...], axis=0)
    mean = jnp.sum(every, axis=0, keepdims=True) * (1.0 / 64)
    off = jnp.where((sub < 4)[None], rb[...] - mean[None], 0.0)
    var = jnp.sum(jnp.sum(off * off, axis=0), axis=0, keepdims=True) * (1.0 / 64)
    norm_out[...] = (own - mean) / jnp.sqrt(var + 1e-06)

    for ch in range(NC):
        for col in (0, 1):
            arrived(gb[col * NC + ch].at[pl.ds(0, 63)], send_sem.at[col, ch])
    for n, buf in ((0, nbuf), (1, mbuf)):
        for k in range(3):
            arrived(buf.at[0], ag_send.at[n, k])
    for g in range(GA):
        arrived(s1a.at[g], ea_send.at[0, g])
        arrived(s2a.at[g], ea_send.at[1, g])
    for g in range(GF):
        arrived(s1f.at[g], ef_send.at[0, g])
        arrived(s2f.at[g], ef_send.at[1, g])
    arrived(ra.at[pl.ds(0, 15)], rw_send.at[0])
    arrived(rb.at[pl.ds(0, 15)], rw_send.at[1])


def layer(pos, lengths, rel_bias, hidden, gains, srcs):
    hbm = pl.BlockSpec(memory_space=pl.ANY)
    vm = pl.BlockSpec(memory_space=pltpu.VMEM)
    sm = pl.BlockSpec(memory_space=pltpu.SMEM)
    dma = pltpu.SemaphoreType.DMA
    v = pltpu.VMEM
    scratch = [v((64, 32, n), BF) for _ in range(2) for n in CH]
    scratch += [
        v((4, ROWS, D), BF), v((4, ROWS, D), BF), v((8, 3, ROWS, ROWS), F32), v((2, LEN, 768), BF),
        v((LEN, 512), BF), v((LEN, 1280), BF), v((4, ROWS, D), F32), v((ROWS, D), F32),
    ]
    for g in (GA, GF):
        w = D // g
        scratch += [v((g, 2, ROWS, w), BF), v((g, 2, ROWS, w), BF), v((g, ROWS, w), BF), v((g, ROWS, w), BF)]
    scratch += [v((16, 8, 128), F32), v((16, 8, 128), F32)]
    scratch += [dma((2, NC)), dma((2, NC, 7)), dma((2, NC)), dma((2, 3)), dma((2, 3))]
    scratch += [dma((2, GA)), dma((2, GA)), dma((2, GF)), dma((2, GF)), dma((2,)), dma((2,))]
    return pl.pallas_call(
        layer_kernel,
        out_shape=(jax.ShapeDtypeStruct((ROWS, D), F32), jax.ShapeDtypeStruct((8, 128), F32)),
        in_specs=[sm, sm, sm, vm, vm] + [hbm] * (2 * NC),
        out_specs=(vm, vm),
        scratch_shapes=scratch,
        compiler_params=pltpu.CompilerParams(
            collective_id=0, has_side_effects=True, vmem_limit_bytes=67043328
        ),
        name="layer",
    )(pos, lengths, rel_bias, hidden, gains, *srcs)


def local(
    hidden_states, lengths, shard_order, gain_attn, w_query, w_key, w_value, w_out, rel_bias, gain_ff,
    w_gate, w_up, w_down, gain_final, w_reward,
):
    ids = jnp.arange(64, dtype=jnp.int32)
    inverse = jnp.sum(ids[:, None] * (shard_order[:, None] == ids[None, :]).astype(jnp.int32), axis=0)
    zs, xs, ys = inverse // 16, (inverse // 4) % 4, inverse % 4
    pos = jnp.stack([ys * 16 + xs * 4 + zs, xs * 16 + ys * 4 + zs])
    gains = jnp.stack([gain_attn, gain_ff, gain_final, w_reward])
    out_t, down_t = w_out.T, w_down.T
    srcs = []
    for col in (0, 1):
        a = slice(col * 256, col * 256 + 256)
        big = (w_gate, w_up)[col]
        srcs += [
            jnp.concatenate([w_query[:, a], w_key[:, a], w_value[:, a]], axis=1), out_t[:, a],
            big[:, :768], big[:, 768:], down_t[:, col * 640 : col * 640 + 640],
        ]
    rows, normalized = layer(pos, lengths, rel_bias, hidden_states, gains, srcs)
    return rows, normalized[0, :1]


def solution(mesh):
    placed = (
        P(("dp", "tensor"), None), P("dp"), P(), P(), P("dp", "tensor"), P("dp", "tensor"), P("dp", "tensor"),
        P("tensor", "dp"), P(None, "tensor"), P(), P("dp", "tensor"), P("dp", "tensor"), P("tensor", "dp"),
        P(), P(),
    )
    return jax.shard_map(
        local, mesh=mesh, in_specs=placed, out_specs=(P(("dp", "tensor"), None), P("dp")), check_vma=False
    )
```

```python
import jax
import jax.numpy as jnp
from jax import lax
from jax.sharding import PartitionSpec as P
from jax.experimental import pallas as pl
from jax.experimental.pallas import tpu as pltpu

DK = 64
LEN = 512
D = 2048
ROWS = 128
MESH = pl.DeviceIdType.MESH
BF = jnp.bfloat16
F32 = jnp.float32
CH = (768, 256, 768, 512, 384, 256)
NC = len(CH)
GA, GF = 2, 4
bucket_edges = (12, 16, 23, 32, 46, 64, 91)


def coords():
    d = lax.axis_index("dp")
    t = lax.axis_index("tensor")
    return d // 16, (d // 4) % 4, d % 4, t // 2, t % 2


def did(z, x, y, h, c):
    return {"dp": z * 16 + x * 4 + y, "tensor": h * 2 + c}


def rms(v, gain):
    return v * lax.rsqrt(jnp.mean(v * v, axis=-1, keepdims=True) + 1e-06) * gain


def nt(a, b):
    return lax.dot_general(a, b, (((1,), (1,)), ((), ())), preferred_element_type=F32)


def layer_kernel(*refs):
    (pos, length_ref, rel, hidden, gains, wq, wk, wv, wgate, wup, wt), refs = refs[:11], refs[11:]
    (out, norm_out), refs = refs[:2], refs[2:]
    gb, refs = refs[: 2 * NC], refs[2 * NC :]
    (nbuf, mbuf, bias, qkv, ctx, act, part, mid, s1a, r1a, s2a, r2a, s1f, r1f, s2f, r2f, ra, rb) = refs[:18]
    send_sem, recv_sem, loc_sem, ag_send, ag_recv, ea_send, ea_recv, ef_send, ef_recv, rw_send, rw_recv = refs[18:]
    z, x, y, h, c = coords()
    me = h * 2 + c
    sib, far = did(z, x, y, h, 1 - c), did(z, x, y, 1 - h, c)
    i_sib, i_far, i_farsib = h * 2 + 1 - c, (1 - h) * 2 + c, (1 - h) * 2 + 1 - c
    length = length_ref[0]

    line = h * 8 + z * 2 + c
    plane = x * 4 + y

    def line_peer(k):
        i = (line + k) % 16
        return did((i // 2) % 4, x, y, i // 8, i % 2)

    def plane_peer(k):
        i = (plane + k) % 16
        return did(z, i // 4, i % 4, h, c)

    base = (y * 16 + x * 4, x * 16 + y * 4)

    def pieces(col, ch):
        a = slice(col * 256, col * 256 + 256)
        big = (wgate, wup)[col]
        if ch == 0:
            return [wq.at[:, a], wk.at[:, a], wv.at[:, a]]
        if ch == 1:
            return [wt.at[:, a]]
        if ch in (2, 3):
            return [big.at[:, slice(0, 768) if ch == 2 else slice(768, 1280)]]
        at = 512 + col * 640
        return [wt.at[:, slice(at, at + 384) if ch == 4 else slice(at + 384, at + 640)]]

    for ch in range(NC):
        for col in (0, 1):
            at = 0
            for piece in pieces(col, ch):
                n = piece.shape[1]
                here = gb[col * NC + ch].at[base[col] + z, :, at : at + n]
                pltpu.make_async_copy(piece, here, loc_sem.at[col, ch]).start()
                at += n

    barrier = pltpu.get_barrier_semaphore()
    for k in range(1, 16):
        pl.semaphore_signal(barrier, inc=1, device_id=line_peer(k), device_id_type=MESH)
        pl.semaphore_signal(barrier, inc=1, device_id=plane_peer(k), device_id_type=MESH)
    pl.semaphore_wait(barrier, 30)

    ring1, ring2 = (x, y), (y, x)

    def remote(s, d, ss, rs, dev):
        return pltpu.make_async_remote_copy(
            src_ref=s, dst_ref=d, send_sem=ss, recv_sem=rs, device_id=dev, device_id_type=MESH
        )

    def ring_peer(col, ph, k):
        if (col == 0) == (ph == 1):
            return did(z, (x + k) % 4, y, h, c)
        return did(z, x, (y + k) % 4, h, c)

    def section(col, ph, k):
        if ph == 1:
            return ring2[col] * 16 + ((ring1[col] + k) % 4) * 4
        return ((ring2[col] + k) % 4) * 16

    def send(col, ch, start, size, slot, dev):
        g = gb[col * NC + ch]
        s = g.at[pl.ds(start, size)]
        remote(s, s, send_sem.at[col, ch], recv_sem.at[col, ch, slot], dev).start()

    def arrived(ref, sem):
        pltpu.make_async_copy(ref, ref, sem).wait()

    def came(col, ch, slot, size):
        arrived(gb[col * NC + ch].at[pl.ds(0, size)], recv_sem.at[col, ch, slot])

    def level(col, ch, lv):
        if lv == 0:
            mine = gb[col * NC + ch].at[base[col] + z]
            arrived(mine, loc_sem.at[col, ch])
            for k in (1, 3, 2):
                remote(
                    mine, mine, send_sem.at[col, ch], recv_sem.at[col, ch, 0], did((z + k) % 4, x, y, h, c)
                ).start()
        elif lv in (1, 3):
            ph = 1 if lv == 1 else 2
            came(col, ch, 0 if ph == 1 else 3, 3 if ph == 1 else 4)
            size, b = (4, 1) if ph == 1 else (16, 4)
            for j, k in ((0, 1), (1, 3)):
                send(col, ch, section(col, ph, 0), size, b + j, ring_peer(col, ph, k))
        elif lv in (2, 4):
            ph = 1 if lv == 2 else 2
            size, b = (4, 1) if ph == 1 else (16, 4)
            half = size // 2
            came(col, ch, b, size)
            send(col, ch, section(col, ph, 3), half, b + 2, ring_peer(col, ph, 1))
            came(col, ch, b + 1, size)
            send(col, ch, section(col, ph, 1) + half, half, b + 2, ring_peer(col, ph, 3))
        else:
            came(col, ch, 6, 16)

    def events(*steps):
        for ch, lv in steps:
            for col in (0, 1):
                level(col, ch, lv)

    def spread(buf, n):
        to_sib = remote(buf.at[me], buf.at[me], ag_send.at[n, 0], ag_recv.at[n, 0], sib)
        to_far = remote(buf.at[me], buf.at[me], ag_send.at[n, 1], ag_recv.at[n, 1], far)
        to_far.start()
        to_sib.start()

    def pass_on(buf, n):
        arrived(buf.at[0], ag_recv.at[n, 1])
        remote(buf.at[i_far], buf.at[i_far], ag_send.at[n, 2], ag_recv.at[n, 2], sib).start()

    def spread_end(buf, n):
        arrived(buf.at[0], ag_recv.at[n, 0])
        arrived(buf.at[0], ag_recv.at[n, 2])

    def to_sibling(which, g, width, s1, r1, ss, rs):
        cols = slice(g * width, (g + 1) * width)
        s1[which, g] = part[(i_sib, i_farsib)[which], :, cols].astype(BF)
        remote(s1.at[which, g], r1.at[which, g], ss.at[which, g], rs.at[which, g], sib).start()

    def to_far(g, width, r1, s2, r2, ss, rs):
        cols = slice(g * width, (g + 1) * width)
        arrived(r1.at[1, g], rs.at[1, g])
        s2[g] = (part[i_far, :, cols] + r1[1, g].astype(F32)).astype(BF)
        remote(s2.at[g], r2.at[g], ss.at[2, g], rs.at[2, g], far).start()

    def total(g, width, r1, r2, rs):
        cols = slice(g * width, (g + 1) * width)
        arrived(r1.at[0, g], rs.at[0, g])
        arrived(r2.at[g], rs.at[2, g])
        return part[me, :, cols] + r1[0, g].astype(F32) + r2[g].astype(F32)

    def blocks(col, ch, first, count, cols):
        g = gb[col * NC + ch]
        return jnp.concatenate([g[pos[col, first + b], :, cols] for b in range(count)], axis=0)

    events((1, 0), (0, 0))
    nbuf[me] = rms(hidden[...], gains[0:1]).astype(BF)
    events((1, 1), (2, 0), (1, 2), (1, 3), (0, 1), (0, 2), (1, 4), (2, 1))
    spread(nbuf, 0)
    events((0, 3))

    row = lax.broadcasted_iota(jnp.int32, (ROWS, ROWS), 0)
    lane = lax.broadcasted_iota(jnp.int32, (ROWS, ROWS), 1)

    def bias_tile(n, _):
        for o in range(3):
            r = (o - 1) * ROWS + lane - row
            dist = jnp.abs(r)
            low = jnp.minimum(dist, 8)
            for edge in bucket_edges:
                low = low + (dist >= edge).astype(jnp.int32)
            bucket = jnp.where(r > 0, 16, 0) + low
            tile = jnp.zeros((ROWS, ROWS), F32)
            for b in range(32):
                tile = jnp.where(bucket == b, rel[b, n], tile)
            bias[n, o] = tile
        return 0

    lax.fori_loop(0, 8, bias_tile, 0)
    events((3, 0), (2, 2), (0, 4), (2, 3))
    pass_on(nbuf, 0)
    events((4, 0), (5, 0), (3, 1))
    spread_end(nbuf, 0)
    events((0, 5))

    for col in (0, 1):
        def qkv_tile(i, _):
            cols = pl.ds(pl.multiple_of(i * 256, 256), 256)
            w = blocks(col, 0, 0, 64, cols)
            qkv[col, :, cols] = jnp.dot(
                nbuf[...].reshape(LEN, D), w, preferred_element_type=F32
            ).astype(BF)
            return 0

        lax.fori_loop(0, 3, qkv_tile, 0)

    lane_q = lax.broadcasted_iota(jnp.int32, (ROWS, 128), 1)
    key_pos = lax.broadcasted_iota(jnp.int32, (ROWS, LEN), 1)
    valid = key_pos < length

    def heads(p, _):
        col = p // 2
        at = (p % 2) * 128
        q_cols = pl.ds(pl.multiple_of(at, 128), 128)
        k_cols = pl.ds(pl.multiple_of(at + 256, 128), 128)
        v_cols = pl.ds(pl.multiple_of(at + 512, 128), 128)
        keys = qkv[col, :, k_cols]
        values = qkv[col, :, v_cols]
        for qt in range(4):
            q = qkv[col, qt * ROWS : (qt + 1) * ROWS, q_cols]
            got = []
            for hh in (0, 1):
                n = p * 2 + hh
                q_head = jnp.where((lane_q >= 64) == (hh == 1), q, jnp.zeros_like(q))
                s = nt(q_head, keys)
                tiles = []
                for kt in range(4):
                    if abs(kt - qt) <= 1:
                        tiles.append(bias[n, kt - qt + 1])
                    else:
                        tiles.append(jnp.full((ROWS, ROWS), rel[31 if kt > qt else 15, n], F32))
                s = jnp.where(valid, s + jnp.concatenate(tiles, axis=1), -1e30)
                e = jnp.exp(s - jnp.max(s, axis=-1, keepdims=True))
                pr = (e * (1.0 / jnp.sum(e, axis=-1, keepdims=True))).astype(BF)
                got.append(jnp.dot(pr, values, preferred_element_type=F32))
            c_cols = pl.ds(pl.multiple_of(p * 128, 128), 128)
            ctx[qt, :, c_cols] = jnp.where(lane_q < 64, got[0], got[1]).astype(BF)
        return 0

    lax.fori_loop(0, 4, heads, 0)
    events((1, 5), (2, 4), (3, 2), (4, 1), (5, 1))

    rows_far, rows_own = pl.ds((1 - h) * 2, 2), pl.ds(h * 2, 2)

    def out_tile(rows, i):
        cols = pl.ds(pl.multiple_of(i * 256, 256), 256)
        c_ = ctx[rows].reshape(256, 512)
        s = nt(c_[:, :256], blocks(0, 1, i * 8, 8, slice(0, 256)))
        s = s + nt(c_[:, 256:], blocks(1, 1, i * 8, 8, slice(0, 256)))
        part[rows, :, cols] = s.reshape(2, ROWS, 256)
        return 0

    wa = D // GA
    na = 8 // GA
    xa = (s1a, r1a, ea_send, ea_recv)
    for g in range(GA):
        lax.fori_loop(g * na, (g + 1) * na, lambda i, _: out_tile(rows_far, i), 0)
        to_sibling(1, g, wa, *xa)
    for g in range(GA):
        lax.fori_loop(g * na, (g + 1) * na, lambda i, _: out_tile(rows_own, i), 0)
        to_sibling(0, g, wa, *xa)
        to_far(g, wa, r1a, s2a, r2a, ea_send, ea_recv)
    events((3, 3), (2, 5), (4, 2), (5, 2))
    for g in range(GA):
        cols = slice(g * wa, (g + 1) * wa)
        mid[:, cols] = hidden[:, cols] + total(g, wa, r1a, r2a, ea_recv)
    mbuf[me] = rms(mid[...], gains[1:2]).astype(BF)
    spread(mbuf, 1)
    events((3, 4), (4, 3), (5, 3))
    arrived(mbuf.at[0], ag_recv.at[1, 0])

    def feed_tile(rows, ch, i, at):
        cols = pl.ds(pl.multiple_of(i * 256, 256), 256)
        lhs = mbuf[rows].reshape(256, D)
        gate = jnp.dot(lhs, blocks(0, ch, 0, 64, cols), preferred_element_type=F32)
        up = jnp.dot(lhs, blocks(1, ch, 0, 64, cols), preferred_element_type=F32)
        a = (jax.nn.gelu(gate, approximate=True) * up).astype(BF)
        act[rows, :, pl.ds(pl.multiple_of(at + i * 256, 256), 256)] = a.reshape(2, ROWS, 256)
        return 0

    def feed_a(rows):
        lax.fori_loop(0, 3, lambda i, _: feed_tile(rows, 2, i, 0), 0)

    def feed_b(rows):
        lax.fori_loop(0, 2, lambda i, _: feed_tile(rows, 3, i, 768), 0)

    feed_a(rows_own)
    events((3, 5))
    feed_b(rows_own)
    events((4, 4), (5, 4))
    pass_on(mbuf, 1)
    arrived(mbuf.at[0], ag_recv.at[1, 2])
    feed_a(rows_far)
    feed_b(rows_far)
    events((4, 5), (5, 5))

    def down_tile(rows, i):
        cols = pl.ds(pl.multiple_of(i * 256, 256), 256)
        s = None
        for col, ch, at in ((0, 4, 0), (0, 5, 384), (1, 4, 640), (1, 5, 1024)):
            n = CH[ch]
            t = nt(act[rows, :, at : at + n].reshape(256, n), blocks(col, ch, i * 8, 8, slice(0, n)))
            s = t if s is None else s + t
        part[rows, :, cols] = s.reshape(2, ROWS, 256)
        return 0

    wf = D // GF
    nf = 8 // GF
    xf = (s1f, r1f, ef_send, ef_recv)
    for g in range(GF):
        lax.fori_loop(g * nf, (g + 1) * nf, lambda i, _: down_tile(rows_far, i), 0)
        to_sibling(1, g, wf, *xf)
        if g > 0:
            to_far(g - 1, wf, r1f, s2f, r2f, ef_send, ef_recv)
    for g in range(GF):
        lax.fori_loop(g * nf, (g + 1) * nf, lambda i, _: down_tile(rows_own, i), 0)
        to_sibling(0, g, wf, *xf)
        if g == 0:
            to_far(GF - 1, wf, r1f, s2f, r2f, ef_send, ef_recv)
    square = jnp.zeros((ROWS, 1), F32)
    dot = jnp.zeros((ROWS, 1), F32)
    for g in range(GF):
        cols = slice(g * wf, (g + 1) * wf)
        o = mid[:, cols] + total(g, wf, r1f, r2f, ef_recv)
        out[:, cols] = o
        square = square + jnp.sum(o * o, axis=-1, keepdims=True)
        dot = dot + jnp.sum(o * (gains[2:3, cols] * gains[3:4, cols]), axis=-1, keepdims=True)
    score = dot * lax.rsqrt(square * (1.0 / D) + 1e-06)
    at_row = lax.broadcasted_iota(jnp.int32, (ROWS, 1), 0) + me * ROWS
    pooled = jnp.sum(jnp.where(at_row < length, score, 0.0), axis=0, keepdims=True)

    ra[line] = jnp.broadcast_to(pooled / length.astype(F32), (8, 128))
    copies = []
    for k in range(1, 16):
        cp = remote(ra.at[line], ra.at[line], rw_send.at[0], rw_recv.at[0], line_peer(k))
        cp.start()
    arrived(ra.at[pl.ds(0, 15)], rw_recv.at[0])
    sub = lax.broadcasted_iota(jnp.int32, (8, 128), 0)
    tile = jnp.zeros((8, 128), F32)
    for k in range(4):
        tile = jnp.where(sub == k, ra[2 * k] + ra[2 * k + 1] + ra[8 + 2 * k] + ra[9 + 2 * k], tile)
    rb[plane] = tile
    for k in range(1, 16):
        remote(rb.at[plane], rb.at[plane], rw_send.at[1], rw_recv.at[1], plane_peer(k)).start()
    own = ra[2 * z] + ra[2 * z + 1] + ra[8 + 2 * z] + ra[9 + 2 * z]
    arrived(rb.at[pl.ds(0, 15)], rw_recv.at[1])
    every = jnp.sum(rb[...], axis=0)
    mean = jnp.sum(every, axis=0, keepdims=True) * (1.0 / 64)
    off = jnp.where((sub < 4)[None], rb[...] - mean[None], 0.0)
    var = jnp.sum(jnp.sum(off * off, axis=0), axis=0, keepdims=True) * (1.0 / 64)
    norm_out[...] = (own - mean) / jnp.sqrt(var + 1e-06)

    for ch in range(NC):
        for col in (0, 1):
            arrived(gb[col * NC + ch].at[pl.ds(0, 63)], send_sem.at[col, ch])
    for n, buf in ((0, nbuf), (1, mbuf)):
        for k in range(3):
            arrived(buf.at[0], ag_send.at[n, k])
    for n, s1, s2, ss in ((GA, s1a, s2a, ea_send), (GF, s1f, s2f, ef_send)):
        for g in range(n):
            arrived(s1.at[0, g], ss.at[0, g])
            arrived(s1.at[1, g], ss.at[1, g])
            arrived(s2.at[g], ss.at[2, g])
    arrived(ra.at[pl.ds(0, 15)], rw_send.at[0])
    arrived(rb.at[pl.ds(0, 15)], rw_send.at[1])


def layer(pos, lengths, rel_bias, hidden, gains, *weights):
    hbm = pl.BlockSpec(memory_space=pl.ANY)
    vm = pl.BlockSpec(memory_space=pltpu.VMEM)
    sm = pl.BlockSpec(memory_space=pltpu.SMEM)
    dma = pltpu.SemaphoreType.DMA
    v = pltpu.VMEM
    scratch = [v((64, 32, n), BF) for _ in range(2) for n in CH]
    scratch += [
        v((4, ROWS, D), BF), v((4, ROWS, D), BF), v((8, 3, ROWS, ROWS), F32), v((2, LEN, 768), BF),
        v((4, ROWS, 512), BF), v((4, ROWS, 1280), BF), v((4, ROWS, D), F32), v((ROWS, D), F32),
    ]
    for g in (GA, GF):
        w = D // g
        scratch += [v((2, g, ROWS, w), BF), v((2, g, ROWS, w), BF), v((g, ROWS, w), BF), v((g, ROWS, w), BF)]
    scratch += [v((16, 8, 128), F32), v((16, 8, 128), F32)]
    scratch += [dma((2, NC)), dma((2, NC, 7)), dma((2, NC)), dma((2, 3)), dma((2, 3))]
    scratch += [dma((3, GA)), dma((3, GA)), dma((3, GF)), dma((3, GF)), dma((2,)), dma((2,))]
    return pl.pallas_call(
        layer_kernel,
        out_shape=(jax.ShapeDtypeStruct((ROWS, D), F32), jax.ShapeDtypeStruct((8, 128), F32)),
        in_specs=[sm, sm, sm, vm, vm] + [hbm] * 6,
        out_specs=(vm, vm),
        scratch_shapes=scratch,
        compiler_params=pltpu.CompilerParams(
            collective_id=0, has_side_effects=True, vmem_limit_bytes=67043328
        ),
        name="layer",
    )(pos, lengths, rel_bias, hidden, gains, *weights)


def local(
    hidden_states, lengths, shard_order, gain_attn, w_query, w_key, w_value, w_out, rel_bias, gain_ff,
    w_gate, w_up, w_down, gain_final, w_reward,
):
    ids = jnp.arange(64, dtype=jnp.int32)
    inverse = jnp.sum(ids[:, None] * (shard_order[:, None] == ids[None, :]).astype(jnp.int32), axis=0)
    zs, xs, ys = inverse // 16, (inverse // 4) % 4, inverse % 4
    pos = jnp.stack([ys * 16 + xs * 4 + zs, xs * 16 + ys * 4 + zs])
    gains = jnp.stack([gain_attn, gain_ff, gain_final, w_reward])
    wt = jnp.concatenate([w_out, w_down], axis=0).T
    rows, normalized = layer(
        pos, lengths, rel_bias, hidden_states, gains, w_query, w_key, w_value, w_gate, w_up, wt
    )
    return rows, normalized[0, :1]


def solution(mesh):
    placed = (
        P(("dp", "tensor"), None), P("dp"), P(), P(), P("dp", "tensor"), P("dp", "tensor"), P("dp", "tensor"),
        P("tensor", "dp"), P(None, "tensor"), P(), P("dp", "tensor"), P("dp", "tensor"), P("tensor", "dp"),
        P(), P(),
    )
    return jax.shard_map(
        local, mesh=mesh, in_specs=placed, out_specs=(P(("dp", "tensor"), None), P("dp")), check_vma=False
    )
```

```python
import jax
import jax.numpy as jnp
from jax import lax
from jax.sharding import PartitionSpec as P
from jax.experimental import pallas as pl
from jax.experimental.pallas import tpu as pltpu

DK = 64
LEN = 512
D = 2048
ROWS = 128
MESH = pl.DeviceIdType.MESH
BF = jnp.bfloat16
F32 = jnp.float32
CH = ((32, 384), (32, 384), (32, 256), (32, 768), (32, 512), (16, 640), (16, 640))
NC = len(CH)
GA, GF = 2, 4
bucket_edges = (12, 16, 23, 32, 46, 64, 91)


def coords():
    d = lax.axis_index("dp")
    t = lax.axis_index("tensor")
    return d // 16, (d // 4) % 4, d % 4, t // 2, t % 2


def did(z, x, y, h, c):
    return {"dp": z * 16 + x * 4 + y, "tensor": h * 2 + c}


def rms(v, gain):
    return v * lax.rsqrt(jnp.mean(v * v, axis=-1, keepdims=True) + 1e-06) * gain


def nt(a, b):
    return lax.dot_general(a, b, (((1,), (1,)), ((), ())), preferred_element_type=F32)


def layer_kernel(*refs):
    (pos, length_ref, rel, hidden, gain_attn, gain_ff, gain_final, w_reward), refs = refs[:8], refs[8:]
    (wq, wk, wv, wgate, wup, wout, wdown), refs = refs[:7], refs[7:]
    (out_hbm, norm_out), refs = refs[:2], refs[2:]
    gb, refs = refs[: 2 * NC], refs[2 * NC :]
    (nbuf, mbuf, bias, qkv, ctx, act, part, mid, s1a, r1a, s2a, r2a, s1f, r1f, s2f, r2f, ra, rb) = refs[:18]
    (gain_t, gain_p, out), refs = refs[18:21], refs[21:]
    send_sem, recv_sem, loc_sem, ag_send, ag_recv, ea_send, ea_recv, ef_send, ef_recv, rw_send, rw_recv, out_sem = refs
    z, x, y, h, c = coords()
    me = h * 2 + c
    sib, far = did(z, x, y, h, 1 - c), did(z, x, y, 1 - h, c)
    i_sib, i_far, i_farsib = h * 2 + 1 - c, (1 - h) * 2 + c, (1 - h) * 2 + 1 - c
    length = length_ref[0]

    line = h * 8 + z * 2 + c
    plane = x * 4 + y

    def line_peer(k):
        i = (line + k) % 16
        return did((i // 2) % 4, x, y, i // 8, i % 2)

    def plane_peer(k):
        i = (plane + k) % 16
        return did(z, i // 4, i % 4, h, c)

    base = (y * 16 + x * 4, x * 16 + y * 4)

    def pieces(col, ch):
        big = (wgate, wup)[col]
        if ch in (0, 1):
            at = col * 256 + ch * 128
            return [w.at[:, at : at + 128] for w in (wq, wk, wv)]
        if ch == 2:
            return [wout.at[:, col * 256 : col * 256 + 256]]
        if ch in (3, 4):
            return [big.at[:, slice(0, 768) if ch == 3 else slice(768, 1280)]]
        return [wdown.at[slice(0, 16) if ch == 5 else slice(16, 32), col * 640 : col * 640 + 640]]

    for ch in range(NC):
        for col in (0, 1):
            at = 0
            for piece in pieces(col, ch):
                n = piece.shape[1]
                here = gb[col * NC + ch].at[base[col] + z, :, at : at + n]
                pltpu.make_async_copy(piece, here, loc_sem.at[col, ch]).start()
                at += n

    barrier = pltpu.get_barrier_semaphore()
    for k in range(1, 16):
        pl.semaphore_signal(barrier, inc=1, device_id=line_peer(k), device_id_type=MESH)
        pl.semaphore_signal(barrier, inc=1, device_id=plane_peer(k), device_id_type=MESH)
    pl.semaphore_wait(barrier, 30)

    ring1, ring2 = (x, y), (y, x)

    def remote(s, d, ss, rs, dev):
        return pltpu.make_async_remote_copy(
            src_ref=s, dst_ref=d, send_sem=ss, recv_sem=rs, device_id=dev, device_id_type=MESH
        )

    def ring_peer(col, ph, k):
        if (col == 0) == (ph == 1):
            return did(z, (x + k) % 4, y, h, c)
        return did(z, x, (y + k) % 4, h, c)

    def section(col, ph, k):
        if ph == 1:
            return ring2[col] * 16 + ((ring1[col] + k) % 4) * 4
        return ((ring2[col] + k) % 4) * 16

    def send(col, ch, start, size, slot, dev):
        g = gb[col * NC + ch]
        s = g.at[pl.ds(start, size)]
        remote(s, s, send_sem.at[col, ch], recv_sem.at[col, ch, slot], dev).start()

    def arrived(ref, sem):
        pltpu.make_async_copy(ref, ref, sem).wait()

    def came(col, ch, slot, size):
        arrived(gb[col * NC + ch].at[pl.ds(0, size)], recv_sem.at[col, ch, slot])

    def level(col, ch, lv):
        if lv == 0:
            mine = gb[col * NC + ch].at[base[col] + z]
            arrived(mine, loc_sem.at[col, ch])
            for k in (1, 3, 2):
                remote(
                    mine, mine, send_sem.at[col, ch], recv_sem.at[col, ch, 0], did((z + k) % 4, x, y, h, c)
                ).start()
        elif lv in (1, 3):
            ph = 1 if lv == 1 else 2
            came(col, ch, 0 if ph == 1 else 3, 3 if ph == 1 else 4)
            size, b = (4, 1) if ph == 1 else (16, 4)
            for j, k in ((0, 1), (1, 3)):
                send(col, ch, section(col, ph, 0), size, b + j, ring_peer(col, ph, k))
        elif lv in (2, 4):
            ph = 1 if lv == 2 else 2
            size, b = (4, 1) if ph == 1 else (16, 4)
            half = size // 2
            came(col, ch, b, size)
            send(col, ch, section(col, ph, 3), half, b + 2, ring_peer(col, ph, 1))
            came(col, ch, b + 1, size)
            send(col, ch, section(col, ph, 1) + half, half, b + 2, ring_peer(col, ph, 3))
        else:
            came(col, ch, 6, 16)

    def events(*steps):
        for ch, lv in steps:
            for col in (0, 1):
                level(col, ch, lv)

    def spread(buf, n):
        to_sib = remote(buf.at[me], buf.at[me], ag_send.at[n, 0], ag_recv.at[n, 0], sib)
        to_far = remote(buf.at[me], buf.at[me], ag_send.at[n, 1], ag_recv.at[n, 1], far)
        to_far.start()
        to_sib.start()

    def pass_on(buf, n):
        arrived(buf.at[0], ag_recv.at[n, 1])
        remote(buf.at[i_far], buf.at[i_far], ag_send.at[n, 2], ag_recv.at[n, 2], sib).start()

    def spread_end(buf, n):
        arrived(buf.at[0], ag_recv.at[n, 0])
        arrived(buf.at[0], ag_recv.at[n, 2])

    def to_sibling(which, g, width, s1, r1, ss, rs):
        cols = slice(g * width, (g + 1) * width)
        s1[which, g] = part[(i_sib, i_farsib)[which], :, cols].astype(BF)
        remote(s1.at[which, g], r1.at[which, g], ss.at[which, g], rs.at[which, g], sib).start()

    def to_far(g, width, r1, s2, r2, ss, rs):
        cols = slice(g * width, (g + 1) * width)
        arrived(r1.at[1, g], rs.at[1, g])
        s2[g] = (part[i_far, :, cols] + r1[1, g].astype(F32)).astype(BF)
        remote(s2.at[g], r2.at[g], ss.at[2, g], rs.at[2, g], far).start()

    def total(g, width, r1, r2, rs):
        cols = slice(g * width, (g + 1) * width)
        arrived(r1.at[0, g], rs.at[0, g])
        arrived(r2.at[g], rs.at[2, g])
        return part[me, :, cols] + r1[0, g].astype(F32) + r2[g].astype(F32)

    def blocks(col, ch, first, count, cols, rows=slice(None)):
        g = gb[col * NC + ch]
        return jnp.concatenate([g[pos[col, first + b], rows, cols] for b in range(count)], axis=0)

    def pick(k):
        i = lax.broadcasted_iota(jnp.int32, (256, 128), 0)
        j = lax.broadcasted_iota(jnp.int32, (256, 128), 1)
        return (i == (j // 16) * 32 + k * 16 + j % 16).astype(F32)

    def halves_first(ref, put):
        for k in (0, 1):
            p = pick(k)
            for v in range(8):
                t = jnp.dot(ref[:, v * 256 : v * 256 + 256], p, precision=lax.Precision.HIGHEST, preferred_element_type=F32)
                put(slice(k * 1024 + v * 128, k * 1024 + v * 128 + 128), t)

    row = lax.broadcasted_iota(jnp.int32, (ROWS, ROWS), 0)
    lane = lax.broadcasted_iota(jnp.int32, (ROWS, ROWS), 1)

    def bias_tile(n, _):
        for o in range(3):
            r = (o - 1) * ROWS + lane - row
            dist = jnp.abs(r)
            low = jnp.minimum(dist, 8)
            for edge in bucket_edges:
                low = low + (dist >= edge).astype(jnp.int32)
            bucket = jnp.where(r > 0, 16, 0) + low
            tile = jnp.zeros((ROWS, ROWS), F32)
            for b in range(32):
                tile = jnp.where(bucket == b, rel[n, b], tile)
            bias[n, o] = tile
        return 0

    def bias_half():
        lax.fori_loop(0, 4, bias_tile, 0)

    pl.when(c == 1)(bias_half)
    events((0, 0))
    nbuf[me] = rms(hidden[...], gain_attn[...]).astype(BF)
    events((0, 1), (1, 0), (2, 0), (0, 2), (1, 1))
    spread(nbuf, 0)
    events((3, 0), (0, 3), (1, 2))
    pl.when(c == 0)(bias_half)
    lax.fori_loop(4, 8, bias_tile, 0)

    def put_mid(cols, t):
        mid[:, cols] = t

    def put_gain(cols, t):
        gain_p[:, cols] = t

    halves_first(hidden, put_mid)
    gain_t[0:1] = gain_ff[...]
    gain_t[1:2] = gain_final[...] * w_reward[...]
    gain_t[2:8] = jnp.zeros((6, D), F32)
    halves_first(gain_t, put_gain)
    events((0, 4), (1, 3), (2, 1), (2, 2))
    pass_on(nbuf, 0)
    events((3, 1))
    spread_end(nbuf, 0)
    events((4, 0), (5, 0), (6, 0), (0, 5))

    def project(ch):
        for col in (0, 1):
            w = blocks(col, ch, 0, 64, slice(0, 384))
            t = jnp.dot(nbuf[...].reshape(LEN, D), w, preferred_element_type=F32)
            qkv[col * 2 + ch] = t.astype(BF)

    lane_q = lax.broadcasted_iota(jnp.int32, (ROWS, 128), 1)
    key_pos = lax.broadcasted_iota(jnp.int32, (ROWS, LEN), 1)
    valid = key_pos < length

    def heads(p, _):
        keys = qkv[p, :, 128:256]
        values = qkv[p, :, 256:384]
        for qt in range(4):
            q = qkv[p, qt * ROWS : (qt + 1) * ROWS, 0:128]
            got = []
            for hh in (0, 1):
                n = p * 2 + hh
                q_head = jnp.where((lane_q >= 64) == (hh == 1), q, jnp.zeros_like(q))
                s = nt(q_head, keys)
                tiles = []
                for kt in range(4):
                    if abs(kt - qt) <= 1:
                        tiles.append(bias[n, kt - qt + 1])
                    else:
                        tiles.append(jnp.full((ROWS, ROWS), rel[n, 31 if kt > qt else 15], F32))
                s = jnp.where(valid, s + jnp.concatenate(tiles, axis=1), -1e30)
                e = jnp.exp(s - jnp.max(s, axis=-1, keepdims=True))
                pr = (e * (1.0 / jnp.sum(e, axis=-1, keepdims=True))).astype(BF)
                got.append(jnp.dot(pr, values, preferred_element_type=F32))
            c_cols = pl.ds(pl.multiple_of(p * 128, 128), 128)
            ctx[qt, :, c_cols] = jnp.where(lane_q < 64, got[0], got[1]).astype(BF)
        return 0

    def pair(i, _):
        return heads((i % 2) * 2 + i // 2, 0)

    project(0)
    events((1, 4), (2, 3))
    lax.fori_loop(0, 1, pair, 0)
    events((3, 2))
    lax.fori_loop(1, 2, pair, 0)
    events((1, 5))
    project(1)
    lax.fori_loop(2, 3, pair, 0)
    events((2, 4), (3, 3))
    lax.fori_loop(3, 4, pair, 0)
    events((4, 1), (2, 5))

    rows_far, rows_own = pl.ds((1 - h) * 2, 2), pl.ds(h * 2, 2)

    def out_tile(rows, k, i):
        cols = pl.ds(pl.multiple_of(k * 1024 + i * 256, 256), 256)
        c_ = ctx[rows].reshape(256, 512)
        r = slice(k * 16, k * 16 + 16)
        s = nt(c_[:, :256], blocks(0, 2, i * 16, 16, slice(0, 256), r))
        s = s + nt(c_[:, 256:], blocks(1, 2, i * 16, 16, slice(0, 256), r))
        part[rows, :, cols] = s.reshape(2, ROWS, 256)
        return 0

    wa = D // GA
    xa = (s1a, r1a, ea_send, ea_recv)
    for g in range(GA):
        lax.fori_loop(0, 4, lambda i, _: out_tile(rows_far, g, i), 0)
        to_sibling(1, g, wa, *xa)
    for g in range(GA):
        lax.fori_loop(0, 4, lambda i, _: out_tile(rows_own, g, i), 0)
        to_sibling(0, g, wa, *xa)
        to_far(g, wa, r1a, s2a, r2a, ea_send, ea_recv)
    events((5, 1), (6, 1), (4, 2), (3, 4), (5, 2), (6, 2), (4, 3), (5, 3))
    for g in range(GA):
        cols = slice(g * wa, (g + 1) * wa)
        mid[:, cols] = mid[:, cols] + total(g, wa, r1a, r2a, ea_recv)
    mbuf[me] = rms(mid[...], gain_p[0:1]).astype(BF)
    spread(mbuf, 1)
    events((3, 5))
    arrived(mbuf.at[0], ag_recv.at[1, 0])

    def feed_tile(rows, ch, i, at):
        cols = pl.ds(pl.multiple_of(i * 256, 256), 256)
        lhs = mbuf[rows].reshape(256, D)

        def both(col):
            return jnp.concatenate([blocks(col, ch, 0, 64, cols, slice(k, k + 16)) for k in (0, 16)], axis=0)

        gate = jnp.dot(lhs, both(0), preferred_element_type=F32)
        up = jnp.dot(lhs, both(1), preferred_element_type=F32)
        a = (jax.nn.gelu(gate, approximate=True) * up).astype(BF)
        act[rows, :, pl.ds(pl.multiple_of(at + i * 256, 256), 256)] = a.reshape(2, ROWS, 256)
        return 0

    def feed_a(rows):
        lax.fori_loop(0, 3, lambda i, _: feed_tile(rows, 3, i, 0), 0)

    def feed_b(rows):
        lax.fori_loop(0, 2, lambda i, _: feed_tile(rows, 4, i, 768), 0)

    feed_a(rows_own)
    events((4, 4), (5, 4), (6, 3))
    pass_on(mbuf, 1)
    arrived(mbuf.at[0], ag_recv.at[1, 2])
    feed_a(rows_far)
    events((4, 5))
    feed_b(rows_far)
    events((5, 5))

    def down_tile(rows, k, i):
        cols = pl.ds(pl.multiple_of(k * 1024 + i * 256, 256), 256)
        a = act[rows].reshape(256, 1280)
        s = nt(a[:, :640], blocks(0, 5 + k, i * 16, 16, slice(0, 640)))
        s = s + nt(a[:, 640:], blocks(1, 5 + k, i * 16, 16, slice(0, 640)))
        part[rows, :, cols] = s.reshape(2, ROWS, 256)
        return 0

    wf = D // GF
    xf = (s1f, r1f, ef_send, ef_recv)

    def down_far(g):
        lax.fori_loop((g % 2) * 2, (g % 2) * 2 + 2, lambda i, _: down_tile(rows_far, g // 2, i), 0)
        to_sibling(1, g, wf, *xf)

    def down_own(g):
        lax.fori_loop((g % 2) * 2, (g % 2) * 2 + 2, lambda i, _: down_tile(rows_own, g // 2, i), 0)
        to_sibling(0, g, wf, *xf)

    down_far(0)
    down_far(1)
    to_far(0, wf, r1f, s2f, r2f, ef_send, ef_recv)
    to_far(1, wf, r1f, s2f, r2f, ef_send, ef_recv)
    events((6, 4))
    feed_b(rows_own)
    down_own(0)
    down_own(1)
    events((6, 5))
    down_far(2)
    down_far(3)
    to_far(2, wf, r1f, s2f, r2f, ef_send, ef_recv)
    down_own(2)
    to_far(3, wf, r1f, s2f, r2f, ef_send, ef_recv)
    down_own(3)
    square = jnp.zeros((ROWS, 1), F32)
    dot = jnp.zeros((ROWS, 1), F32)
    for g in range(GF):
        cols = slice(g * wf, (g + 1) * wf)
        o = mid[:, cols] + total(g, wf, r1f, r2f, ef_recv)
        p = pick(g // 2)
        for q in range(4):
            v = (g % 2) * 4 + q
            t = lax.dot_general(o[:, q * 128 : q * 128 + 128], p, (((1,), (1,)), ((), ())),
                                precision=lax.Precision.HIGHEST, preferred_element_type=F32)
            to = slice(v * 256, v * 256 + 256)
            out[:, to] = t if g < 2 else out[:, to] + t
        square = square + jnp.sum(o * o, axis=-1, keepdims=True)
        dot = dot + jnp.sum(o * gain_p[1:2, cols], axis=-1, keepdims=True)
    score = dot * lax.rsqrt(square * (1.0 / D) + 1e-06)
    at_row = lax.broadcasted_iota(jnp.int32, (ROWS, 1), 0) + me * ROWS
    pooled = jnp.sum(jnp.where(at_row < length, score, 0.0), axis=0, keepdims=True)

    result = pltpu.make_async_copy(out, out_hbm, out_sem)
    result.start()

    ra[line] = jnp.broadcast_to(pooled / length.astype(F32), (8, 128))
    copies = []
    for k in range(1, 16):
        cp = remote(ra.at[line], ra.at[line], rw_send.at[0], rw_recv.at[0], line_peer(k))
        cp.start()
    arrived(ra.at[pl.ds(0, 15)], rw_recv.at[0])
    sub = lax.broadcasted_iota(jnp.int32, (8, 128), 0)
    tile = jnp.zeros((8, 128), F32)
    for k in range(4):
        tile = jnp.where(sub == k, ra[2 * k] + ra[2 * k + 1] + ra[8 + 2 * k] + ra[9 + 2 * k], tile)
    rb[plane] = tile
    for k in range(1, 16):
        remote(rb.at[plane], rb.at[plane], rw_send.at[1], rw_recv.at[1], plane_peer(k)).start()
    own = ra[2 * z] + ra[2 * z + 1] + ra[8 + 2 * z] + ra[9 + 2 * z]
    arrived(rb.at[pl.ds(0, 15)], rw_recv.at[1])
    every = jnp.sum(rb[...], axis=0)
    mean = jnp.sum(every, axis=0, keepdims=True) * (1.0 / 64)
    off = jnp.where((sub < 4)[None], rb[...] - mean[None], 0.0)
    var = jnp.sum(jnp.sum(off * off, axis=0), axis=0, keepdims=True) * (1.0 / 64)
    norm_out[...] = ((own - mean) / jnp.sqrt(var + 1e-06))[0:1, 0:1]

    for ch in range(NC):
        for col in (0, 1):
            arrived(gb[col * NC + ch].at[pl.ds(0, 63)], send_sem.at[col, ch])
    for n, buf in ((0, nbuf), (1, mbuf)):
        for k in range(3):
            arrived(buf.at[0], ag_send.at[n, k])
    for n, s1, s2, ss in ((GA, s1a, s2a, ea_send), (GF, s1f, s2f, ef_send)):
        for g in range(n):
            arrived(s1.at[0, g], ss.at[0, g])
            arrived(s1.at[1, g], ss.at[1, g])
            arrived(s2.at[g], ss.at[2, g])
    arrived(ra.at[pl.ds(0, 15)], rw_send.at[0])
    arrived(rb.at[pl.ds(0, 15)], rw_send.at[1])
    result.wait()


def layer(pos, lengths, rel_bias, hidden, *arrays):
    hbm = pl.BlockSpec(memory_space=pl.ANY)
    vm = pl.BlockSpec(memory_space=pltpu.VMEM)
    sm = pl.BlockSpec(memory_space=pltpu.SMEM)
    dma = pltpu.SemaphoreType.DMA
    v = pltpu.VMEM
    scratch = [v((64, r, n), BF) for _ in range(2) for r, n in CH]
    scratch += [
        v((4, ROWS, D), BF), v((4, ROWS, D), BF), v((8, 3, ROWS, ROWS), F32), v((4, LEN, 384), BF),
        v((4, ROWS, 512), BF), v((4, ROWS, 1280), BF), v((4, ROWS, D), F32), v((ROWS, D), F32),
    ]
    for g in (GA, GF):
        w = D // g
        scratch += [v((2, g, ROWS, w), BF), v((2, g, ROWS, w), BF), v((g, ROWS, w), BF), v((g, ROWS, w), BF)]
    scratch += [v((16, 8, 128), F32), v((16, 8, 128), F32), v((8, D), F32), v((8, D), F32), v((ROWS, D), F32)]
    scratch += [dma((2, NC)), dma((2, NC, 7)), dma((2, NC)), dma((2, 3)), dma((2, 3))]
    scratch += [dma((3, GA)), dma((3, GA)), dma((3, GF)), dma((3, GF)), dma((2,)), dma((2,)), dma]
    return pl.pallas_call(
        layer_kernel,
        out_shape=(jax.ShapeDtypeStruct((ROWS, D), F32), jax.ShapeDtypeStruct((1, 1), F32)),
        in_specs=[sm, sm, sm] + [vm] * 5 + [hbm] * 7,
        out_specs=(hbm, vm),
        scratch_shapes=scratch,
        compiler_params=pltpu.CompilerParams(
            collective_id=0, has_side_effects=True, vmem_limit_bytes=56 << 20
        ),
        name="layer",
    )(pos, lengths, rel_bias, hidden, *arrays)


def local(
    hidden_states, lengths, shard_order, gain_attn, w_query, w_key, w_value, w_out, rel_bias, gain_ff,
    w_gate, w_up, w_down, gain_final, w_reward,
):
    ids = jnp.arange(64, dtype=jnp.int32)
    zs, xs, ys = ids // 16, (ids // 4) % 4, ids % 4
    half = jnp.arange(2, dtype=jnp.int32)[:, None, None]
    slot = jnp.where(half == 0, ys * 16 + xs * 4, xs * 16 + ys * 4) + zs
    pos = jnp.sum(jnp.where(shard_order[None, None, :] == ids[None, :, None], slot, 0), axis=2)
    rows, normalized = layer(
        pos, lengths, rel_bias.T, hidden_states,
        gain_attn.reshape(1, D), gain_ff.reshape(1, D), gain_final.reshape(1, D), w_reward.reshape(1, D),
        w_query, w_key, w_value, w_gate, w_up, w_out.T, w_down.T,
    )
    return rows, normalized.reshape(1)


def solution(mesh):
    placed = (
        P(("dp", "tensor"), None), P("dp"), P(), P(), P("dp", "tensor"), P("dp", "tensor"), P("dp", "tensor"),
        P("tensor", "dp"), P(None, "tensor"), P(), P("dp", "tensor"), P("dp", "tensor"), P("tensor", "dp"),
        P(), P(),
    )
    return jax.shard_map(
        local, mesh=mesh, in_specs=placed, out_specs=(P(("dp", "tensor"), None), P("dp")), check_vma=False
    )
```

```python
import jax
import jax.numpy as jnp
from jax import lax
from jax.sharding import PartitionSpec as P
from jax.experimental import pallas as pl
from jax.experimental.pallas import tpu as pltpu

DK = 64
LEN = 512
D = 2048
ROWS = 128
MESH = pl.DeviceIdType.MESH
BF = jnp.bfloat16
F32 = jnp.float32
CH = ((32, 384), (32, 384), (32, 256), (32, 768), (32, 512), (16, 640), (16, 640))
NC = len(CH)
GA, GF = 2, 4
bucket_edges = (12, 16, 23, 32, 46, 64, 91)


def coords():
    d = lax.axis_index("dp")
    t = lax.axis_index("tensor")
    return d // 16, (d // 4) % 4, d % 4, t // 2, t % 2


def did(z, x, y, h, c):
    return {"dp": z * 16 + x * 4 + y, "tensor": h * 2 + c}


def rms(v, gain):
    return v * lax.rsqrt(jnp.mean(v * v, axis=-1, keepdims=True) + 1e-06) * gain


def nt(a, b):
    return lax.dot_general(a, b, (((1,), (1,)), ((), ())), preferred_element_type=F32)


def layer_kernel(*refs):
    (pos, length_ref, rel, hidden, gain_attn, gain_ff, gain_final, w_reward), refs = refs[:8], refs[8:]
    (wq, wk, wv, wgate, wup, wout, wdown), refs = refs[:7], refs[7:]
    (out_hbm, norm_out), refs = refs[:2], refs[2:]
    gb, refs = refs[: 2 * NC], refs[2 * NC :]
    (nbuf, mbuf, bias, qkv, ctx, act, part, mid, s1a, r1a, s2a, r2a, s1f, r1f, s2f, r2f, ra, rb) = refs[:18]
    (gain_t, gain_p, out), refs = refs[18:21], refs[21:]
    send_sem, recv_sem, loc_sem, ag_send, ag_recv, ea_send, ea_recv, ef_send, ef_recv, rw_send, rw_recv, out_sem = refs
    z, x, y, h, c = coords()
    me = h * 2 + c
    sib, far = did(z, x, y, h, 1 - c), did(z, x, y, 1 - h, c)
    i_sib, i_far, i_farsib = h * 2 + 1 - c, (1 - h) * 2 + c, (1 - h) * 2 + 1 - c
    length = length_ref[0]

    line = h * 8 + z * 2 + c
    plane = x * 4 + y

    def line_peer(k):
        i = (line + k) % 16
        return did((i // 2) % 4, x, y, i // 8, i % 2)

    def plane_peer(k):
        i = (plane + k) % 16
        return did(z, i // 4, i % 4, h, c)

    base = (y * 16 + x * 4, x * 16 + y * 4)

    def pieces(col, ch):
        big = (wgate, wup)[col]
        if ch in (0, 1):
            at = col * 256 + ch * 128
            return [w.at[:, at : at + 128] for w in (wq, wk, wv)]
        if ch == 2:
            return [wout.at[:, col * 256 : col * 256 + 256]]
        if ch in (3, 4):
            return [big.at[:, slice(0, 768) if ch == 3 else slice(768, 1280)]]
        return [wdown.at[slice(0, 16) if ch == 5 else slice(16, 32), col * 640 : col * 640 + 640]]

    for ch in range(NC):
        for col in (0, 1):
            at = 0
            for piece in pieces(col, ch):
                n = piece.shape[1]
                here = gb[col * NC + ch].at[base[col] + z, :, at : at + n]
                pltpu.make_async_copy(piece, here, loc_sem.at[col, ch]).start()
                at += n

    barrier = pltpu.get_barrier_semaphore()
    for k in range(1, 16):
        pl.semaphore_signal(barrier, inc=1, device_id=line_peer(k), device_id_type=MESH)
        pl.semaphore_signal(barrier, inc=1, device_id=plane_peer(k), device_id_type=MESH)
    pl.semaphore_wait(barrier, 30)

    ring1, ring2 = (x, y), (y, x)

    def remote(s, d, ss, rs, dev):
        return pltpu.make_async_remote_copy(
            src_ref=s, dst_ref=d, send_sem=ss, recv_sem=rs, device_id=dev, device_id_type=MESH
        )

    def ring_peer(col, ph, k):
        if (col == 0) == (ph == 1):
            return did(z, (x + k) % 4, y, h, c)
        return did(z, x, (y + k) % 4, h, c)

    def section(col, ph, k):
        if ph == 1:
            return ring2[col] * 16 + ((ring1[col] + k) % 4) * 4
        return ((ring2[col] + k) % 4) * 16

    def send(col, ch, start, size, slot, dev):
        g = gb[col * NC + ch]
        s = g.at[pl.ds(start, size)]
        remote(s, s, send_sem.at[col, ch], recv_sem.at[col, ch, slot], dev).start()

    def arrived(ref, sem):
        pltpu.make_async_copy(ref, ref, sem).wait()

    def came(col, ch, slot, size):
        arrived(gb[col * NC + ch].at[pl.ds(0, size)], recv_sem.at[col, ch, slot])

    def level(col, ch, lv):
        if lv == 0:
            mine = gb[col * NC + ch].at[base[col] + z]
            arrived(mine, loc_sem.at[col, ch])
            for k in (1, 3, 2):
                remote(
                    mine, mine, send_sem.at[col, ch], recv_sem.at[col, ch, 0], did((z + k) % 4, x, y, h, c)
                ).start()
        elif lv in (1, 3):
            ph = 1 if lv == 1 else 2
            came(col, ch, 0 if ph == 1 else 3, 3 if ph == 1 else 4)
            size, b = (4, 1) if ph == 1 else (16, 4)
            for j, k in ((0, 1), (1, 3)):
                send(col, ch, section(col, ph, 0), size, b + j, ring_peer(col, ph, k))
        elif lv in (2, 4):
            ph = 1 if lv == 2 else 2
            size, b = (4, 1) if ph == 1 else (16, 4)
            half = size // 2
            came(col, ch, b, size)
            send(col, ch, section(col, ph, 3), half, b + 2, ring_peer(col, ph, 1))
            came(col, ch, b + 1, size)
            send(col, ch, section(col, ph, 1) + half, half, b + 2, ring_peer(col, ph, 3))
        else:
            came(col, ch, 6, 16)

    def events(*steps):
        for ch, lv in steps:
            for col in (0, 1):
                level(col, ch, lv)

    def spread(buf, n):
        to_sib = remote(buf.at[me], buf.at[me], ag_send.at[n, 0], ag_recv.at[n, 0], sib)
        to_far = remote(buf.at[me], buf.at[me], ag_send.at[n, 1], ag_recv.at[n, 1], far)
        to_far.start()
        to_sib.start()

    def pass_on(buf, n):
        arrived(buf.at[0], ag_recv.at[n, 1])
        remote(buf.at[i_far], buf.at[i_far], ag_send.at[n, 2], ag_recv.at[n, 2], sib).start()

    def spread_end(buf, n):
        arrived(buf.at[0], ag_recv.at[n, 0])
        arrived(buf.at[0], ag_recv.at[n, 2])

    def to_sibling(which, g, width, s1, r1, ss, rs):
        cols = slice(g * width, (g + 1) * width)
        s1[which, g] = part[(i_sib, i_farsib)[which], :, cols].astype(BF)
        remote(s1.at[which, g], r1.at[which, g], ss.at[which, g], rs.at[which, g], sib).start()

    def to_far(g, width, r1, s2, r2, ss, rs):
        cols = slice(g * width, (g + 1) * width)
        arrived(r1.at[1, g], rs.at[1, g])
        s2[g] = (part[i_far, :, cols] + r1[1, g].astype(F32)).astype(BF)
        remote(s2.at[g], r2.at[g], ss.at[2, g], rs.at[2, g], far).start()

    def total(g, width, r1, r2, rs):
        cols = slice(g * width, (g + 1) * width)
        arrived(r1.at[0, g], rs.at[0, g])
        arrived(r2.at[g], rs.at[2, g])
        return part[me, :, cols] + r1[0, g].astype(F32) + r2[g].astype(F32)

    def blocks(col, ch, first, count, cols, rows=slice(None)):
        g = gb[col * NC + ch]
        return jnp.concatenate([g[pos[col, first + b], rows, cols] for b in range(count)], axis=0)

    def pick(k):
        i = lax.broadcasted_iota(jnp.int32, (256, 128), 0)
        j = lax.broadcasted_iota(jnp.int32, (256, 128), 1)
        return (i == (j // 16) * 32 + k * 16 + j % 16).astype(F32)

    def halves_first(ref, put):
        for k in (0, 1):
            p = pick(k)
            for v in range(8):
                t = jnp.dot(ref[:, v * 256 : v * 256 + 256], p, precision=lax.Precision.HIGHEST, preferred_element_type=F32)
                put(slice(k * 1024 + v * 128, k * 1024 + v * 128 + 128), t)

    row = lax.broadcasted_iota(jnp.int32, (ROWS, ROWS), 0)
    lane = lax.broadcasted_iota(jnp.int32, (ROWS, ROWS), 1)

    def bias_tile(n, _):
        for o in range(3):
            r = (o - 1) * ROWS + lane - row
            dist = jnp.abs(r)
            low = jnp.minimum(dist, 8)
            for edge in bucket_edges:
                low = low + (dist >= edge).astype(jnp.int32)
            bucket = jnp.where(r > 0, 16, 0) + low
            tile = jnp.zeros((ROWS, ROWS), F32)
            for b in range(32):
                tile = jnp.where(bucket == b, rel[n, b], tile)
            bias[n, o] = tile
        return 0

    def bias_half():
        lax.fori_loop(0, 4, bias_tile, 0)

    pl.when(c == 1)(bias_half)
    events((0, 0))
    nbuf[me] = rms(hidden[...], gain_attn[...]).astype(BF)
    events((0, 1), (1, 0), (2, 0), (0, 2), (1, 1))
    spread(nbuf, 0)
    events((3, 0), (0, 3), (1, 2))
    pl.when(c == 0)(bias_half)
    lax.fori_loop(4, 8, bias_tile, 0)

    def put_mid(cols, t):
        mid[:, cols] = t

    def put_gain(cols, t):
        gain_p[:, cols] = t

    halves_first(hidden, put_mid)
    gain_t[0:1] = gain_ff[...]
    gain_t[1:2] = gain_final[...] * w_reward[...]
    gain_t[2:8] = jnp.zeros((6, D), F32)
    halves_first(gain_t, put_gain)
    events((0, 4), (1, 3), (2, 1), (2, 2))
    pass_on(nbuf, 0)
    events((3, 1))
    spread_end(nbuf, 0)
    events((4, 0), (5, 0), (6, 0), (0, 5))

    def project(ch):
        for col in (0, 1):
            w = blocks(col, ch, 0, 64, slice(0, 384))
            t = jnp.dot(nbuf[...].reshape(LEN, D), w, preferred_element_type=F32)
            qkv[col * 2 + ch] = t.astype(BF)

    lane_q = lax.broadcasted_iota(jnp.int32, (ROWS, 128), 1)
    key_pos = lax.broadcasted_iota(jnp.int32, (ROWS, LEN), 1)
    valid = key_pos < length

    def heads(p, _):
        keys = qkv[p, :, 128:256]
        values = qkv[p, :, 256:384]
        for qt in range(4):
            q = qkv[p, qt * ROWS : (qt + 1) * ROWS, 0:128]
            got = []
            for hh in (0, 1):
                n = p * 2 + hh
                q_head = jnp.where((lane_q >= 64) == (hh == 1), q, jnp.zeros_like(q))
                s = nt(q_head, keys)
                tiles = []
                for kt in range(4):
                    if abs(kt - qt) <= 1:
                        tiles.append(bias[n, kt - qt + 1])
                    else:
                        tiles.append(jnp.full((ROWS, ROWS), rel[n, 31 if kt > qt else 15], F32))
                s = jnp.where(valid, s + jnp.concatenate(tiles, axis=1), -1e30)
                e = jnp.exp(s - jnp.max(s, axis=-1, keepdims=True))
                pr = (e * (1.0 / jnp.sum(e, axis=-1, keepdims=True))).astype(BF)
                got.append(jnp.dot(pr, values, preferred_element_type=F32))
            c_cols = pl.ds(pl.multiple_of(p * 128, 128), 128)
            ctx[qt, :, c_cols] = jnp.where(lane_q < 64, got[0], got[1]).astype(BF)
        return 0

    def pair(i, _):
        return heads((i % 2) * 2 + i // 2, 0)

    project(0)
    events((1, 4), (2, 3))
    lax.fori_loop(0, 1, pair, 0)
    events((3, 2))
    lax.fori_loop(1, 2, pair, 0)
    events((1, 5))
    project(1)
    lax.fori_loop(2, 3, pair, 0)
    events((2, 4), (3, 3))
    lax.fori_loop(3, 4, pair, 0)
    events((4, 1), (5, 1), (6, 1), (2, 5))

    rows_far, rows_own = pl.ds((1 - h) * 2, 2), pl.ds(h * 2, 2)

    def out_tile(rows, k, i):
        cols = pl.ds(pl.multiple_of(k * 1024 + i * 256, 256), 256)
        c_ = ctx[rows].reshape(256, 512)
        r = slice(k * 16, k * 16 + 16)
        s = nt(c_[:, :256], blocks(0, 2, i * 16, 16, slice(0, 256), r))
        s = s + nt(c_[:, 256:], blocks(1, 2, i * 16, 16, slice(0, 256), r))
        part[rows, :, cols] = s.reshape(2, ROWS, 256)
        return 0

    wa = D // GA
    xa = (s1a, r1a, ea_send, ea_recv)
    for g in range(GA):
        lax.fori_loop(0, 4, lambda i, _: out_tile(rows_far, g, i), 0)
        to_sibling(1, g, wa, *xa)
    for g in range(GA):
        lax.fori_loop(0, 4, lambda i, _: out_tile(rows_own, g, i), 0)
        to_sibling(0, g, wa, *xa)
        to_far(g, wa, r1a, s2a, r2a, ea_send, ea_recv)
    events((4, 2), (5, 2), (6, 2), (3, 4), (4, 3), (5, 3))
    for g in range(GA):
        cols = slice(g * wa, (g + 1) * wa)
        mid[:, cols] = mid[:, cols] + total(g, wa, r1a, r2a, ea_recv)
    mbuf[me] = rms(mid[...], gain_p[0:1]).astype(BF)
    spread(mbuf, 1)
    events((3, 5))
    arrived(mbuf.at[0], ag_recv.at[1, 0])

    def feed_tile(rows, ch, i, at):
        cols = pl.ds(pl.multiple_of(i * 256, 256), 256)
        lhs = mbuf[rows].reshape(256, D)

        def both(col):
            return jnp.concatenate([blocks(col, ch, 0, 64, cols, slice(k, k + 16)) for k in (0, 16)], axis=0)

        gate = jnp.dot(lhs, both(0), preferred_element_type=F32)
        up = jnp.dot(lhs, both(1), preferred_element_type=F32)
        a = (jax.nn.gelu(gate, approximate=True) * up).astype(BF)
        act[rows, :, pl.ds(pl.multiple_of(at + i * 256, 256), 256)] = a.reshape(2, ROWS, 256)
        return 0

    def feed_a(rows):
        lax.fori_loop(0, 3, lambda i, _: feed_tile(rows, 3, i, 0), 0)

    def feed_b(rows):
        lax.fori_loop(0, 2, lambda i, _: feed_tile(rows, 4, i, 768), 0)

    feed_a(rows_own)
    events((4, 4), (5, 4), (6, 3))
    pass_on(mbuf, 1)
    arrived(mbuf.at[0], ag_recv.at[1, 2])
    feed_a(rows_far)
    events((4, 5))
    feed_b(rows_far)
    events((5, 5))

    def down_tile(rows, k, i):
        cols = pl.ds(pl.multiple_of(k * 1024 + i * 256, 256), 256)
        a = act[rows].reshape(256, 1280)
        s = nt(a[:, :640], blocks(0, 5 + k, i * 16, 16, slice(0, 640)))
        s = s + nt(a[:, 640:], blocks(1, 5 + k, i * 16, 16, slice(0, 640)))
        part[rows, :, cols] = s.reshape(2, ROWS, 256)
        return 0

    wf = D // GF
    xf = (s1f, r1f, ef_send, ef_recv)

    def down_far(g):
        lax.fori_loop((g % 2) * 2, (g % 2) * 2 + 2, lambda i, _: down_tile(rows_far, g // 2, i), 0)
        to_sibling(1, g, wf, *xf)

    def down_own(g):
        lax.fori_loop((g % 2) * 2, (g % 2) * 2 + 2, lambda i, _: down_tile(rows_own, g // 2, i), 0)
        to_sibling(0, g, wf, *xf)

    down_far(0)
    down_far(1)
    to_far(0, wf, r1f, s2f, r2f, ef_send, ef_recv)
    to_far(1, wf, r1f, s2f, r2f, ef_send, ef_recv)
    events((6, 4))
    feed_b(rows_own)
    down_own(0)
    down_own(1)
    events((6, 5))
    down_far(2)
    down_far(3)
    to_far(2, wf, r1f, s2f, r2f, ef_send, ef_recv)
    down_own(2)
    to_far(3, wf, r1f, s2f, r2f, ef_send, ef_recv)
    down_own(3)
    square = jnp.zeros((ROWS, 1), F32)
    dot = jnp.zeros((ROWS, 1), F32)
    for g in range(GF):
        cols = slice(g * wf, (g + 1) * wf)
        o = mid[:, cols] + total(g, wf, r1f, r2f, ef_recv)
        p = pick(g // 2)
        for q in range(4):
            v = (g % 2) * 4 + q
            t = lax.dot_general(o[:, q * 128 : q * 128 + 128], p, (((1,), (1,)), ((), ())),
                                precision=lax.Precision.HIGHEST, preferred_element_type=F32)
            to = slice(v * 256, v * 256 + 256)
            out[:, to] = t if g < 2 else out[:, to] + t
        square = square + jnp.sum(o * o, axis=-1, keepdims=True)
        dot = dot + jnp.sum(o * gain_p[1:2, cols], axis=-1, keepdims=True)
    score = dot * lax.rsqrt(square * (1.0 / D) + 1e-06)
    at_row = lax.broadcasted_iota(jnp.int32, (ROWS, 1), 0) + me * ROWS
    pooled = jnp.sum(jnp.where(at_row < length, score, 0.0), axis=0, keepdims=True)

    result = pltpu.make_async_copy(out, out_hbm, out_sem)
    result.start()

    ra[line] = jnp.broadcast_to(pooled / length.astype(F32), (8, 128))
    copies = []
    for k in range(1, 16):
        cp = remote(ra.at[line], ra.at[line], rw_send.at[0], rw_recv.at[0], line_peer(k))
        cp.start()
    arrived(ra.at[pl.ds(0, 15)], rw_recv.at[0])
    sub = lax.broadcasted_iota(jnp.int32, (8, 128), 0)
    tile = jnp.zeros((8, 128), F32)
    for k in range(4):
        tile = jnp.where(sub == k, ra[2 * k] + ra[2 * k + 1] + ra[8 + 2 * k] + ra[9 + 2 * k], tile)
    rb[plane] = tile
    for k in range(1, 16):
        remote(rb.at[plane], rb.at[plane], rw_send.at[1], rw_recv.at[1], plane_peer(k)).start()
    own = ra[2 * z] + ra[2 * z + 1] + ra[8 + 2 * z] + ra[9 + 2 * z]
    arrived(rb.at[pl.ds(0, 15)], rw_recv.at[1])
    every = jnp.sum(rb[...], axis=0)
    mean = jnp.sum(every, axis=0, keepdims=True) * (1.0 / 64)
    off = jnp.where((sub < 4)[None], rb[...] - mean[None], 0.0)
    var = jnp.sum(jnp.sum(off * off, axis=0), axis=0, keepdims=True) * (1.0 / 64)
    norm_out[...] = ((own - mean) / jnp.sqrt(var + 1e-06))[0:1, 0:1]

    for ch in range(NC):
        for col in (0, 1):
            arrived(gb[col * NC + ch].at[pl.ds(0, 63)], send_sem.at[col, ch])
    for n, buf in ((0, nbuf), (1, mbuf)):
        for k in range(3):
            arrived(buf.at[0], ag_send.at[n, k])
    for n, s1, s2, ss in ((GA, s1a, s2a, ea_send), (GF, s1f, s2f, ef_send)):
        for g in range(n):
            arrived(s1.at[0, g], ss.at[0, g])
            arrived(s1.at[1, g], ss.at[1, g])
            arrived(s2.at[g], ss.at[2, g])
    arrived(ra.at[pl.ds(0, 15)], rw_send.at[0])
    arrived(rb.at[pl.ds(0, 15)], rw_send.at[1])
    result.wait()


def layer(pos, lengths, rel_bias, hidden, *arrays):
    hbm = pl.BlockSpec(memory_space=pl.ANY)
    vm = pl.BlockSpec(memory_space=pltpu.VMEM)
    sm = pl.BlockSpec(memory_space=pltpu.SMEM)
    dma = pltpu.SemaphoreType.DMA
    v = pltpu.VMEM
    scratch = [v((64, r, n), BF) for _ in range(2) for r, n in CH]
    scratch += [
        v((4, ROWS, D), BF), v((4, ROWS, D), BF), v((8, 3, ROWS, ROWS), F32), v((4, LEN, 384), BF),
        v((4, ROWS, 512), BF), v((4, ROWS, 1280), BF), v((4, ROWS, D), F32), v((ROWS, D), F32),
    ]
    for g in (GA, GF):
        w = D // g
        scratch += [v((2, g, ROWS, w), BF), v((2, g, ROWS, w), BF), v((g, ROWS, w), BF), v((g, ROWS, w), BF)]
    scratch += [v((16, 8, 128), F32), v((16, 8, 128), F32), v((8, D), F32), v((8, D), F32), v((ROWS, D), F32)]
    scratch += [dma((2, NC)), dma((2, NC, 7)), dma((2, NC)), dma((2, 3)), dma((2, 3))]
    scratch += [dma((3, GA)), dma((3, GA)), dma((3, GF)), dma((3, GF)), dma((2,)), dma((2,)), dma]
    return pl.pallas_call(
        layer_kernel,
        out_shape=(jax.ShapeDtypeStruct((ROWS, D), F32), jax.ShapeDtypeStruct((1, 1), F32)),
        in_specs=[sm, sm, sm] + [vm] * 5 + [hbm] * 7,
        out_specs=(hbm, vm),
        scratch_shapes=scratch,
        compiler_params=pltpu.CompilerParams(
            collective_id=0, has_side_effects=True, vmem_limit_bytes=56 << 20
        ),
        name="layer",
    )(pos, lengths, rel_bias, hidden, *arrays)


def local(
    hidden_states, lengths, shard_order, gain_attn, w_query, w_key, w_value, w_out, rel_bias, gain_ff,
    w_gate, w_up, w_down, gain_final, w_reward,
):
    ids = jnp.arange(64, dtype=jnp.int32)
    zs, xs, ys = ids // 16, (ids // 4) % 4, ids % 4
    half = jnp.arange(2, dtype=jnp.int32)[:, None, None]
    slot = jnp.where(half == 0, ys * 16 + xs * 4, xs * 16 + ys * 4) + zs
    pos = jnp.sum(jnp.where(shard_order[None, None, :] == ids[None, :, None], slot, 0), axis=2)
    rows, normalized = layer(
        pos, lengths, rel_bias.T, hidden_states,
        gain_attn.reshape(1, D), gain_ff.reshape(1, D), gain_final.reshape(1, D), w_reward.reshape(1, D),
        w_query, w_key, w_value, w_gate, w_up, w_out.T, w_down.T,
    )
    return rows, normalized.reshape(1)


def solution(mesh):
    placed = (
        P(("dp", "tensor"), None), P("dp"), P(), P(), P("dp", "tensor"), P("dp", "tensor"), P("dp", "tensor"),
        P("tensor", "dp"), P(None, "tensor"), P(), P("dp", "tensor"), P("dp", "tensor"), P("tensor", "dp"),
        P(), P(),
    )
    return jax.shard_map(
        local, mesh=mesh, in_specs=placed, out_specs=(P(("dp", "tensor"), None), P("dp")), check_vma=False
    )
```

```python
import jax
import jax.numpy as jnp
from jax import lax
from jax.sharding import PartitionSpec as P
from jax.experimental import pallas as pl
from jax.experimental.pallas import tpu as pltpu

DK = 64
LEN = 512
D = 2048
ROWS = 128
MESH = pl.DeviceIdType.MESH
BF = jnp.bfloat16
F32 = jnp.float32
CH = ((32, 384), (32, 384), (32, 256), (32, 768), (32, 512), (16, 640), (16, 640))
NC = len(CH)
GA, GF = 2, 4
bucket_edges = (12, 16, 23, 32, 46, 64, 91)


def coords():
    d = lax.axis_index("dp")
    t = lax.axis_index("tensor")
    return d // 16, (d // 4) % 4, d % 4, t // 2, t % 2


def did(z, x, y, h, c):
    return {"dp": z * 16 + x * 4 + y, "tensor": h * 2 + c}


def rms(v, gain):
    return v * lax.rsqrt(jnp.mean(v * v, axis=-1, keepdims=True) + 1e-06) * gain


def nt(a, b):
    return lax.dot_general(a, b, (((1,), (1,)), ((), ())), preferred_element_type=F32)


def layer_kernel(*refs):
    (pos, length_ref, rel, hidden, gain_attn, gain_ff, gain_final, w_reward), refs = refs[:8], refs[8:]
    (wq, wk, wv, wgate, wup, wout, wdown), refs = refs[:7], refs[7:]
    (out_hbm, norm_out), refs = refs[:2], refs[2:]
    gb, refs = refs[: 2 * NC], refs[2 * NC :]
    (nbuf, mbuf, bias, qkv, ctx, act, part, mid, s1a, r1a, s2a, r2a, s1f, r1f, s2f, r2f, ra, rb) = refs[:18]
    (gain_t, gain_p, out), refs = refs[18:21], refs[21:]
    send_sem, recv_sem, loc_sem, ag_send, ag_recv, ea_send, ea_recv, ef_send, ef_recv, rw_send, rw_recv, out_sem = refs
    z, x, y, h, c = coords()
    me = h * 2 + c
    sib, far = did(z, x, y, h, 1 - c), did(z, x, y, 1 - h, c)
    i_sib, i_far, i_farsib = h * 2 + 1 - c, (1 - h) * 2 + c, (1 - h) * 2 + 1 - c
    length = length_ref[0]

    line = h * 8 + z * 2 + c
    plane = x * 4 + y

    def line_peer(k):
        i = (line + k) % 16
        return did((i // 2) % 4, x, y, i // 8, i % 2)

    def plane_peer(k):
        i = (plane + k) % 16
        return did(z, i // 4, i % 4, h, c)

    base = (y * 16 + x * 4, x * 16 + y * 4)

    def pieces(col, ch):
        big = (wgate, wup)[col]
        if ch in (0, 1):
            at = col * 256 + ch * 128
            return [w.at[:, at : at + 128] for w in (wq, wk, wv)]
        if ch == 2:
            return [wout.at[:, col * 256 : col * 256 + 256]]
        if ch in (3, 4):
            return [big.at[:, slice(0, 768) if ch == 3 else slice(768, 1280)]]
        return [wdown.at[slice(0, 16) if ch == 5 else slice(16, 32), col * 640 : col * 640 + 640]]

    barrier = pltpu.get_barrier_semaphore()
    for k in (8, 7, 9, 6, 10, 5, 11, 4, 12, 3, 13, 2, 14, 1, 15):
        pl.semaphore_signal(barrier, inc=1, device_id=line_peer(k), device_id_type=MESH)
        pl.semaphore_signal(barrier, inc=1, device_id=plane_peer(k), device_id_type=MESH)
    for ch in range(NC):
        for col in (0, 1):
            at = 0
            for piece in pieces(col, ch):
                n = piece.shape[1]
                here = gb[col * NC + ch].at[base[col] + z, :, at : at + n]
                pltpu.make_async_copy(piece, here, loc_sem.at[col, ch]).start()
                at += n

    pl.semaphore_wait(barrier, 30)

    ring1, ring2 = (x, y), (y, x)

    def remote(s, d, ss, rs, dev):
        return pltpu.make_async_remote_copy(
            src_ref=s, dst_ref=d, send_sem=ss, recv_sem=rs, device_id=dev, device_id_type=MESH
        )

    def ring_peer(col, ph, k):
        if (col == 0) == (ph == 1):
            return did(z, (x + k) % 4, y, h, c)
        return did(z, x, (y + k) % 4, h, c)

    def section(col, ph, k):
        if ph == 1:
            return ring2[col] * 16 + ((ring1[col] + k) % 4) * 4
        return ((ring2[col] + k) % 4) * 16

    def send(col, ch, start, size, slot, dev):
        g = gb[col * NC + ch]
        s = g.at[pl.ds(start, size)]
        remote(s, s, send_sem.at[col, ch], recv_sem.at[col, ch, slot], dev).start()

    def arrived(ref, sem):
        pltpu.make_async_copy(ref, ref, sem).wait()

    def came(col, ch, slot, size):
        arrived(gb[col * NC + ch].at[pl.ds(0, size)], recv_sem.at[col, ch, slot])

    def level(col, ch, lv):
        if lv == 0:
            mine = gb[col * NC + ch].at[base[col] + z]
            arrived(mine, loc_sem.at[col, ch])
            for k in (1, 3, 2):
                remote(
                    mine, mine, send_sem.at[col, ch], recv_sem.at[col, ch, 0], did((z + k) % 4, x, y, h, c)
                ).start()
        elif lv in (1, 3):
            ph = 1 if lv == 1 else 2
            came(col, ch, 0 if ph == 1 else 3, 3 if ph == 1 else 4)
            size, b = (4, 1) if ph == 1 else (16, 4)
            for j, k in ((0, 1), (1, 3)):
                send(col, ch, section(col, ph, 0), size, b + j, ring_peer(col, ph, k))
        elif lv in (2, 4):
            ph = 1 if lv == 2 else 2
            size, b = (4, 1) if ph == 1 else (16, 4)
            half = size // 2
            came(col, ch, b, size)
            send(col, ch, section(col, ph, 3), half, b + 2, ring_peer(col, ph, 1))
            came(col, ch, b + 1, size)
            send(col, ch, section(col, ph, 1) + half, half, b + 2, ring_peer(col, ph, 3))
        else:
            came(col, ch, 6, 16)

    def events(*steps):
        for ch, lv in steps:
            for col in (0, 1):
                level(col, ch, lv)

    def spread(buf, n):
        to_sib = remote(buf.at[me], buf.at[me], ag_send.at[n, 0], ag_recv.at[n, 0], sib)
        to_far = remote(buf.at[me], buf.at[me], ag_send.at[n, 1], ag_recv.at[n, 1], far)
        to_far.start()
        to_sib.start()

    def pass_on(buf, n):
        arrived(buf.at[0], ag_recv.at[n, 1])
        remote(buf.at[i_far], buf.at[i_far], ag_send.at[n, 2], ag_recv.at[n, 2], sib).start()

    def spread_end(buf, n):
        arrived(buf.at[0], ag_recv.at[n, 0])
        arrived(buf.at[0], ag_recv.at[n, 2])

    def to_sibling(which, g, width, s1, r1, ss, rs):
        cols = slice(g * width, (g + 1) * width)
        s1[which, g] = part[(i_sib, i_farsib)[which], :, cols].astype(BF)
        remote(s1.at[which, g], r1.at[which, g], ss.at[which, g], rs.at[which, g], sib).start()

    def to_far(g, width, r1, s2, r2, ss, rs):
        cols = slice(g * width, (g + 1) * width)
        arrived(r1.at[1, g], rs.at[1, g])
        s2[g] = (part[i_far, :, cols] + r1[1, g].astype(F32)).astype(BF)
        remote(s2.at[g], r2.at[g], ss.at[2, g], rs.at[2, g], far).start()

    def total(g, width, r1, r2, rs):
        cols = slice(g * width, (g + 1) * width)
        arrived(r1.at[0, g], rs.at[0, g])
        arrived(r2.at[g], rs.at[2, g])
        return part[me, :, cols] + r1[0, g].astype(F32) + r2[g].astype(F32)

    def blocks(col, ch, first, count, cols, rows=slice(None)):
        g = gb[col * NC + ch]
        return jnp.concatenate([g[pos[col, first + b], rows, cols] for b in range(count)], axis=0)

    def pick(k):
        i = lax.broadcasted_iota(jnp.int32, (256, 128), 0)
        j = lax.broadcasted_iota(jnp.int32, (256, 128), 1)
        return (i == (j // 16) * 32 + k * 16 + j % 16).astype(F32)

    def halves_first(ref, put):
        for k in (0, 1):
            p = pick(k)
            for v in range(8):
                t = jnp.dot(ref[:, v * 256 : v * 256 + 256], p, precision=lax.Precision.HIGHEST, preferred_element_type=F32)
                put(slice(k * 1024 + v * 128, k * 1024 + v * 128 + 128), t)

    row = lax.broadcasted_iota(jnp.int32, (ROWS, ROWS), 0)
    lane = lax.broadcasted_iota(jnp.int32, (ROWS, ROWS), 1)

    def bias_tile(n, _):
        for o in range(3):
            r = (o - 1) * ROWS + lane - row
            dist = jnp.abs(r)
            low = jnp.minimum(dist, 8)
            for edge in bucket_edges:
                low = low + (dist >= edge).astype(jnp.int32)
            bucket = jnp.where(r > 0, 16, 0) + low
            tile = jnp.zeros((ROWS, ROWS), F32)
            for b in range(32):
                tile = jnp.where(bucket == b, rel[n, b], tile)
            bias[n, o] = tile
        return 0

    def bias_half():
        lax.fori_loop(0, 4, bias_tile, 0)

    pl.when(c == 1)(bias_half)
    events((0, 0))
    nbuf[me] = rms(hidden[...], gain_attn[...]).astype(BF)
    events((0, 1), (1, 0), (2, 0), (0, 2), (1, 1))
    spread(nbuf, 0)
    events((3, 0), (0, 3), (1, 2))
    pl.when(c == 0)(bias_half)
    lax.fori_loop(4, 8, bias_tile, 0)

    def put_mid(cols, t):
        mid[:, cols] = t

    def put_gain(cols, t):
        gain_p[:, cols] = t

    halves_first(hidden, put_mid)
    gain_t[0:1] = gain_ff[...]
    gain_t[1:2] = gain_final[...] * w_reward[...]
    gain_t[2:8] = jnp.zeros((6, D), F32)
    halves_first(gain_t, put_gain)
    events((0, 4), (1, 3), (2, 1), (2, 2))
    pass_on(nbuf, 0)
    events((3, 1))
    spread_end(nbuf, 0)
    events((4, 0), (5, 0), (6, 0), (0, 5))

    def project(ch):
        for col in (0, 1):
            w = blocks(col, ch, 0, 64, slice(0, 384))
            t = jnp.dot(nbuf[...].reshape(LEN, D), w, preferred_element_type=F32)
            qkv[col * 2 + ch] = t.astype(BF)

    lane_q = lax.broadcasted_iota(jnp.int32, (ROWS, 128), 1)
    key_pos = lax.broadcasted_iota(jnp.int32, (ROWS, LEN), 1)
    valid = key_pos < length

    def heads(p, _):
        keys = qkv[p, :, 128:256]
        values = qkv[p, :, 256:384]
        for qt in range(4):
            q = qkv[p, qt * ROWS : (qt + 1) * ROWS, 0:128]
            got = []
            for hh in (0, 1):
                n = p * 2 + hh
                q_head = jnp.where((lane_q >= 64) == (hh == 1), q, jnp.zeros_like(q))
                s = nt(q_head, keys)
                tiles = []
                for kt in range(4):
                    if abs(kt - qt) <= 1:
                        tiles.append(bias[n, kt - qt + 1])
                    else:
                        tiles.append(jnp.full((ROWS, ROWS), rel[n, 31 if kt > qt else 15], F32))
                s = jnp.where(valid, s + jnp.concatenate(tiles, axis=1), -1e30)
                e = jnp.exp(s - jnp.max(s, axis=-1, keepdims=True))
                pr = (e * (1.0 / jnp.sum(e, axis=-1, keepdims=True))).astype(BF)
                got.append(jnp.dot(pr, values, preferred_element_type=F32))
            c_cols = pl.ds(pl.multiple_of(p * 128, 128), 128)
            ctx[qt, :, c_cols] = jnp.where(lane_q < 64, got[0], got[1]).astype(BF)
        return 0

    def pair(i, _):
        return heads((i % 2) * 2 + i // 2, 0)

    project(0)
    events((1, 4), (2, 3))
    lax.fori_loop(0, 1, pair, 0)
    events((3, 2))
    lax.fori_loop(1, 2, pair, 0)
    events((1, 5))
    project(1)
    lax.fori_loop(2, 3, pair, 0)
    events((2, 4), (3, 3))
    lax.fori_loop(3, 4, pair, 0)
    events((4, 1), (5, 1), (6, 1), (2, 5))

    rows_far, rows_own = pl.ds((1 - h) * 2, 2), pl.ds(h * 2, 2)

    def out_tile(rows, k, i):
        cols = pl.ds(pl.multiple_of(k * 1024 + i * 256, 256), 256)
        c_ = ctx[rows].reshape(256, 512)
        r = slice(k * 16, k * 16 + 16)
        s = nt(c_[:, :256], blocks(0, 2, i * 16, 16, slice(0, 256), r))
        s = s + nt(c_[:, 256:], blocks(1, 2, i * 16, 16, slice(0, 256), r))
        part[rows, :, cols] = s.reshape(2, ROWS, 256)
        return 0

    wa = D // GA
    xa = (s1a, r1a, ea_send, ea_recv)
    for g in range(GA):
        lax.fori_loop(0, 4, lambda i, _: out_tile(rows_far, g, i), 0)
        to_sibling(1, g, wa, *xa)
    for g in range(GA):
        lax.fori_loop(0, 4, lambda i, _: out_tile(rows_own, g, i), 0)
        to_sibling(0, g, wa, *xa)
        to_far(g, wa, r1a, s2a, r2a, ea_send, ea_recv)
    events((4, 2), (5, 2), (6, 2), (3, 4), (4, 3), (5, 3))
    for g in range(GA):
        cols = slice(g * wa, (g + 1) * wa)
        mid[:, cols] = mid[:, cols] + total(g, wa, r1a, r2a, ea_recv)
    mbuf[me] = rms(mid[...], gain_p[0:1]).astype(BF)
    spread(mbuf, 1)
    events((3, 5))
    arrived(mbuf.at[0], ag_recv.at[1, 0])

    def feed_tile(rows, ch, i, at):
        cols = pl.ds(pl.multiple_of(i * 256, 256), 256)
        lhs = mbuf[rows].reshape(256, D)

        def both(col):
            return jnp.concatenate([blocks(col, ch, 0, 64, cols, slice(k, k + 16)) for k in (0, 16)], axis=0)

        gate = jnp.dot(lhs, both(0), preferred_element_type=F32)
        up = jnp.dot(lhs, both(1), preferred_element_type=F32)
        a = (jax.nn.gelu(gate, approximate=True) * up).astype(BF)
        act[rows, :, pl.ds(pl.multiple_of(at + i * 256, 256), 256)] = a.reshape(2, ROWS, 256)
        return 0

    def feed_a(rows):
        lax.fori_loop(0, 3, lambda i, _: feed_tile(rows, 3, i, 0), 0)

    def feed_b(rows):
        lax.fori_loop(0, 2, lambda i, _: feed_tile(rows, 4, i, 768), 0)

    feed_a(rows_own)
    events((4, 4), (5, 4), (6, 3))
    pass_on(mbuf, 1)
    arrived(mbuf.at[0], ag_recv.at[1, 2])
    feed_a(rows_far)
    events((4, 5))
    feed_b(rows_far)
    events((5, 5))

    def down_tile(rows, k, i):
        cols = pl.ds(pl.multiple_of(k * 1024 + i * 256, 256), 256)
        a = act[rows].reshape(256, 1280)
        s = nt(a[:, :640], blocks(0, 5 + k, i * 16, 16, slice(0, 640)))
        s = s + nt(a[:, 640:], blocks(1, 5 + k, i * 16, 16, slice(0, 640)))
        part[rows, :, cols] = s.reshape(2, ROWS, 256)
        return 0

    wf = D // GF
    xf = (s1f, r1f, ef_send, ef_recv)

    def down_far(g):
        lax.fori_loop((g % 2) * 2, (g % 2) * 2 + 2, lambda i, _: down_tile(rows_far, g // 2, i), 0)
        to_sibling(1, g, wf, *xf)

    def down_own(g):
        lax.fori_loop((g % 2) * 2, (g % 2) * 2 + 2, lambda i, _: down_tile(rows_own, g // 2, i), 0)
        to_sibling(0, g, wf, *xf)

    down_far(0)
    down_far(1)
    to_far(0, wf, r1f, s2f, r2f, ef_send, ef_recv)
    to_far(1, wf, r1f, s2f, r2f, ef_send, ef_recv)
    events((6, 4))
    feed_b(rows_own)
    down_own(0)
    down_own(1)
    events((6, 5))
    down_far(2)
    down_far(3)
    to_far(2, wf, r1f, s2f, r2f, ef_send, ef_recv)
    down_own(2)
    to_far(3, wf, r1f, s2f, r2f, ef_send, ef_recv)
    down_own(3)
    square = jnp.zeros((ROWS, 1), F32)
    dot = jnp.zeros((ROWS, 1), F32)
    for g in range(GF):
        cols = slice(g * wf, (g + 1) * wf)
        o = mid[:, cols] + total(g, wf, r1f, r2f, ef_recv)
        p = pick(g // 2)
        for q in range(4):
            v = (g % 2) * 4 + q
            t = lax.dot_general(o[:, q * 128 : q * 128 + 128], p, (((1,), (1,)), ((), ())),
                                precision=lax.Precision.HIGHEST, preferred_element_type=F32)
            to = slice(v * 256, v * 256 + 256)
            out[:, to] = t if g < 2 else out[:, to] + t
        square = square + jnp.sum(o * o, axis=-1, keepdims=True)
        dot = dot + jnp.sum(o * gain_p[1:2, cols], axis=-1, keepdims=True)
    score = dot * lax.rsqrt(square * (1.0 / D) + 1e-06)
    at_row = lax.broadcasted_iota(jnp.int32, (ROWS, 1), 0) + me * ROWS
    pooled = jnp.sum(jnp.where(at_row < length, score, 0.0), axis=0, keepdims=True)

    result = pltpu.make_async_copy(out, out_hbm, out_sem)
    result.start()

    ra[line] = jnp.broadcast_to(pooled / length.astype(F32), (8, 128))
    copies = []
    for k in range(1, 16):
        cp = remote(ra.at[line], ra.at[line], rw_send.at[0], rw_recv.at[0], line_peer(k))
        cp.start()
    arrived(ra.at[pl.ds(0, 15)], rw_recv.at[0])
    sub = lax.broadcasted_iota(jnp.int32, (8, 128), 0)
    tile = jnp.zeros((8, 128), F32)
    for k in range(4):
        tile = jnp.where(sub == k, ra[2 * k] + ra[2 * k + 1] + ra[8 + 2 * k] + ra[9 + 2 * k], tile)
    rb[plane] = tile
    for k in range(1, 16):
        remote(rb.at[plane], rb.at[plane], rw_send.at[1], rw_recv.at[1], plane_peer(k)).start()
    own = ra[2 * z] + ra[2 * z + 1] + ra[8 + 2 * z] + ra[9 + 2 * z]
    arrived(rb.at[pl.ds(0, 15)], rw_recv.at[1])
    every = jnp.sum(rb[...], axis=0)
    mean = jnp.sum(every, axis=0, keepdims=True) * (1.0 / 64)
    off = jnp.where((sub < 4)[None], rb[...] - mean[None], 0.0)
    var = jnp.sum(jnp.sum(off * off, axis=0), axis=0, keepdims=True) * (1.0 / 64)
    norm_out[...] = ((own - mean) / jnp.sqrt(var + 1e-06))[0:1, 0:1]

    for ch in range(NC):
        for col in (0, 1):
            arrived(gb[col * NC + ch].at[pl.ds(0, 63)], send_sem.at[col, ch])
    for n, buf in ((0, nbuf), (1, mbuf)):
        for k in range(3):
            arrived(buf.at[0], ag_send.at[n, k])
    for n, s1, s2, ss in ((GA, s1a, s2a, ea_send), (GF, s1f, s2f, ef_send)):
        for g in range(n):
            arrived(s1.at[0, g], ss.at[0, g])
            arrived(s1.at[1, g], ss.at[1, g])
            arrived(s2.at[g], ss.at[2, g])
    arrived(ra.at[pl.ds(0, 15)], rw_send.at[0])
    arrived(rb.at[pl.ds(0, 15)], rw_send.at[1])
    result.wait()


def layer(pos, lengths, rel_bias, hidden, *arrays):
    hbm = pl.BlockSpec(memory_space=pl.ANY)
    vm = pl.BlockSpec(memory_space=pltpu.VMEM)
    sm = pl.BlockSpec(memory_space=pltpu.SMEM)
    dma = pltpu.SemaphoreType.DMA
    v = pltpu.VMEM
    scratch = [v((64, r, n), BF) for _ in range(2) for r, n in CH]
    scratch += [
        v((4, ROWS, D), BF), v((4, ROWS, D), BF), v((8, 3, ROWS, ROWS), F32), v((4, LEN, 384), BF),
        v((4, ROWS, 512), BF), v((4, ROWS, 1280), BF), v((4, ROWS, D), F32), v((ROWS, D), F32),
    ]
    for g in (GA, GF):
        w = D // g
        scratch += [v((2, g, ROWS, w), BF), v((2, g, ROWS, w), BF), v((g, ROWS, w), BF), v((g, ROWS, w), BF)]
    scratch += [v((16, 8, 128), F32), v((16, 8, 128), F32), v((8, D), F32), v((8, D), F32), v((ROWS, D), F32)]
    scratch += [dma((2, NC)), dma((2, NC, 7)), dma((2, NC)), dma((2, 3)), dma((2, 3))]
    scratch += [dma((3, GA)), dma((3, GA)), dma((3, GF)), dma((3, GF)), dma((2,)), dma((2,)), dma]
    return pl.pallas_call(
        layer_kernel,
        out_shape=(jax.ShapeDtypeStruct((ROWS, D), F32), jax.ShapeDtypeStruct((1, 1), F32)),
        in_specs=[sm, sm, sm] + [vm] * 5 + [hbm] * 7,
        out_specs=(hbm, vm),
        scratch_shapes=scratch,
        compiler_params=pltpu.CompilerParams(
            collective_id=0, has_side_effects=True, vmem_limit_bytes=56 << 20
        ),
        name="layer",
    )(pos, lengths, rel_bias, hidden, *arrays)


def local(
    hidden_states, lengths, shard_order, gain_attn, w_query, w_key, w_value, w_out, rel_bias, gain_ff,
    w_gate, w_up, w_down, gain_final, w_reward,
):
    ids = jnp.arange(64, dtype=jnp.int32)
    zs, xs, ys = ids // 16, (ids // 4) % 4, ids % 4
    half = jnp.arange(2, dtype=jnp.int32)[:, None, None]
    slot = jnp.where(half == 0, ys * 16 + xs * 4, xs * 16 + ys * 4) + zs
    pos = jnp.sum(jnp.where(shard_order[None, None, :] == ids[None, :, None], slot, 0), axis=2)
    rows, normalized = layer(
        pos, lengths, rel_bias.T, hidden_states,
        gain_attn.reshape(1, D), gain_ff.reshape(1, D), gain_final.reshape(1, D), w_reward.reshape(1, D),
        w_query, w_key, w_value, w_gate, w_up, w_out.T, w_down.T,
    )
    return rows, normalized.reshape(1)


def solution(mesh):
    placed = (
        P(("dp", "tensor"), None), P("dp"), P(), P(), P("dp", "tensor"), P("dp", "tensor"), P("dp", "tensor"),
        P("tensor", "dp"), P(None, "tensor"), P(), P("dp", "tensor"), P("dp", "tensor"), P("tensor", "dp"),
        P(), P(),
    )
    return jax.shard_map(
        local, mesh=mesh, in_specs=placed, out_specs=(P(("dp", "tensor"), None), P("dp")), check_vma=False
    )
```
